32 devices in a mesh: leaf: 8 (over y, x, core), rhs: 4 (over z).
Axes of the slice: x: 2, y: 2, z: 4, core: 2. Of those that a mesh axis runs over, the one named last changes fastest.
Arguments:
- charges: bfloat16 [65536, 2048], P(('leaf', 'rhs')), may hold values from -6 to 6
- leaf_coef: bfloat16 [128, 256, 512], P(('leaf', 'rhs')), may hold values from -0.25 to 0.25
- leaf_rows: int32 [128, 256], P(('leaf', 'rhs')), may hold values from 0 to 511, as said below
- local_interp: bfloat16 [120, 256, 512], P('leaf'), may hold values from -0.25 to 0.25
- top_interp: bfloat16 [1792, 512], P('leaf'), may hold values from -0.25 to 0.25
Outputs:
- subtree_skel: bfloat16 [2048, 2048], P('leaf', 'rhs')
- top_skel: bfloat16 [1792, 2048], P('leaf', 'rhs')
The draws below stay inside these ranges and needn't reach their ends.
Inputs may be any that keep to these rules, and one draw needn't show every extreme that they name: `leaf_rows`: each row holds 256 distinct positions.
All inputs are finite; a program needn't handle non-finite values.
Results may differ from the reference program's by a relative error of at most 0.012.
Values may be sent and summed in bfloat16 or wider, within the bound.
A program may use at most 64 MiB of HBM per device.

```python
import jax
import jax.numpy as jnp
from jax import lax

S = 256
M = 512
LEAVES_DEV = 16
LEAVES = 128
COLS = 2048
PACK = 224
N_LEAF = 8


def draw_leaf_rows(key, part):
    scores = jax.random.randint(key, (LEAVES, M), 0, 1 << 20) * M + jnp.arange(M, dtype=jnp.int32)[None, :]
    order = jnp.argsort(scores, axis=1, stable=True)
    return order[:, :S].astype(jnp.int32)


def steps_of(own_key, dims, cuts, low, high):
    gain, own = 1.0, jax.random.fold_in(own_key, 6)
    for axis_at, parts in cuts:
        steps = jnp.exp(jax.random.uniform(jax.random.fold_in(own, axis_at), (parts,), jnp.float32, low / len(cuts), high / len(cuts)))
        gain = gain * jnp.repeat(steps, dims[axis_at] // parts).reshape([-1 if axis == axis_at else 1 for axis in range(len(dims))])
    return gain


def scatter_about(own_key, shape, scale, limit, cuts=(), kind=jnp.bfloat16):
    entries = jax.random.normal(own_key, shape, jnp.float32) * scale
    if len(cuts) > 0:
        entries = steps_of(own_key, shape, cuts, -0.22, 0.18) * entries
    return jnp.clip(entries, min=-limit, max=limit).astype(kind)


def setup_inputs(seed: int = 0) -> dict:
    arg_keys = jax.random.split(jax.random.key(seed), 6)
    return {
        "charges": scatter_about(arg_keys[0], (LEAVES * M, COLS), 1.0, 6.0, ((0, 32),)),
        "leaf_coef": scatter_about(arg_keys[1], (LEAVES, S, M), M ** -0.5, 0.25, ((0, 32),)),
        "leaf_rows": draw_leaf_rows(jax.random.fold_in(arg_keys[5], 71), 0),
        "local_interp": scatter_about(arg_keys[3], (N_LEAF * (LEAVES_DEV - 1), S, 2 * S), (2 * S) ** -0.5, 0.25, ((0, 8),)),
        "top_interp": scatter_about(arg_keys[4], (N_LEAF * PACK, 2 * S), (2 * S) ** -0.5, 0.25, ((0, 8),)),
    }


def pick_rows(block, chosen):
    return block[chosen]


def subtree(operand):
    points, coef, chosen, interp = operand
    picked = jax.vmap(pick_rows)(points, chosen).astype(jnp.float32)
    mixed = jnp.einsum("nsm,nmc->nsc", coef.astype(jnp.float32), points.astype(jnp.float32))
    skeleton = (picked + mixed).astype(jnp.bfloat16)
    offset = 0
    node_count = LEAVES_DEV
    while node_count > 1:
        node_count = node_count // 2
        stacked = skeleton.reshape(node_count, 2 * S, COLS)
        matrices = interp[offset:offset + node_count]
        skeleton = jnp.einsum("nij,njc->nic", matrices.astype(jnp.float32), stacked.astype(jnp.float32)).astype(jnp.bfloat16)
        offset = offset + node_count
    return skeleton[0]


def reference(charges, leaf_coef, leaf_rows, local_interp, top_interp):
    points = charges.reshape(N_LEAF, LEAVES_DEV, M, COLS)
    coef = leaf_coef.reshape(N_LEAF, LEAVES_DEV, S, M)
    chosen = leaf_rows.reshape(N_LEAF, LEAVES_DEV, S)
    interp = local_interp.reshape(N_LEAF, LEAVES_DEV - 1, S, 2 * S)
    roots = lax.map(subtree, (points, coef, chosen, interp))
    blocks = top_interp.reshape(N_LEAF, PACK, 2 * S)
    top_levels = N_LEAF.bit_length() - 1
    skeleton = roots
    pieces = []
    for level in range(1, top_levels + 1):
        row_count = S >> level
        offset = S - (S >> (level - 1))
        node_count = N_LEAF >> level
        matrices = blocks[:, offset:offset + row_count].reshape(node_count, S, 2 * S)
        stacked = skeleton.reshape(node_count, 2 * S, COLS)
        skeleton = jnp.einsum("nij,njc->nic", matrices.astype(jnp.float32), stacked.astype(jnp.float32)).astype(jnp.bfloat16)
        pieces.append(skeleton.reshape(N_LEAF, row_count, COLS))
    top_skel = jnp.concatenate(pieces, axis=1).reshape(N_LEAF * PACK, COLS)
    return roots.reshape(N_LEAF * S, COLS), top_skel
```

```python
import functools

import jax
import jax.numpy as jnp
from jax import lax
from jax.experimental import pallas as pl
from jax.experimental.pallas import tpu as pltpu
from jax.sharding import PartitionSpec as P

PIECE = 128
CHUNK = 256
LAG = 2
AHEAD = 5
MESH = pl.DeviceIdType.MESH


def bit(value, k):
    return (value // (1 << k)) % 2


def flip(value, offset, bits):
    out = 0
    for k in range(bits):
        a, b = bit(value, k), bit(offset, k)
        out = out + (a + b - 2 * a * b) * (1 << k)
    return out


def chosen(z, table):
    size = len(table)
    if len(set(table)) == 1:
        return table[0]
    out = 0
    for k, value in enumerate(table):
        differs = ((z - k + size) % size + size - 1) // size
        out = out + (1 - differs) * value
    return out


def dot(a, b):
    return jnp.dot(a, b, preferred_element_type=jnp.float32)


def up_block(R, i):
    return R - 1 - i


def block_order(R, Q, z):
    when = {}
    for c in range(R):
        if c > z:
            when[c] = LAG * z + (R - 1 - c) * Q
        elif c < z:
            when[c] = LAG * (R - 1 - z) + c * Q
        else:
            when[c] = final_step(R, Q, z)
    first = (lambda c: -c) if z < R / 2 else (lambda c: c)
    return sorted(range(R), key=lambda c: (c == z, when[c], first(c)))


def final_step(R, Q, z):
    below = LAG * z + (R - 1 - z) * Q if z > 0 else 0
    above = LAG * (R - 1 - z) + z * Q if z < R - 1 else 0
    return max(below, above)


def segments(S, L, n_leaf):
    out, start = [], 0
    for delta in range(n_leaf):
        first = max(delta.bit_length(), 1)
        rows = (S >> first - 1) - (S >> L)
        padded = -(-rows // 32) * 32
        out.append((start, first, rows, padded))
        start += padded
    return out, start


def kernel(plan, charges, coef, rows, interp, top, root_out, top_out, *scratch):
    (points, mats, picks, nodes, halves, ops, skel, leafw, tops, tables, wide, level_ops, parts,
     below, above, leaving, coming, load_sem, up_send, up_recv, down_send, down_recv,
     table_send, table_recv, part_send, part_recv) = scratch
    R, L, H, Q = plan["R"], plan["L"], plan["H"], plan["Q"]
    leaves, S, M = plan["leaves"], plan["S"], plan["M"]
    m, n_leaf, early = plan["m"], plan["n_leaf"], plan["early"]
    pack = top.shape[0]
    total = leaves * R
    bf = jnp.bfloat16
    z = lax.axis_index("rhs")
    p = lax.axis_index("leaf")
    segs, height = segments(S, L, n_leaf)
    orders = [block_order(R, Q, k) for k in range(R)]
    chunks = R * H

    barrier = pltpu.get_barrier_semaphore()
    if R > 1:
        @pl.when(z > 0)
        def _():
            pl.semaphore_signal(barrier, inc=1, device_id={"rhs": z - 1}, device_id_type=MESH)

        @pl.when(z < R - 1)
        def _():
            pl.semaphore_signal(barrier, inc=1, device_id={"rhs": z + 1}, device_id_type=MESH)
    for delta in range(1, n_leaf):
        pl.semaphore_signal(barrier, inc=1, device_id={"leaf": flip(p, delta, L)}, device_id_type=MESH)
    neighbours = chosen(z, [(k > 0) + (k < R - 1) for k in range(R)])

    def block(i):
        return chosen(z, [orders[k][i] for k in range(R)])

    def chunk_copy(i):
        column = (block(i // H) * H + i % H) * CHUNK
        return pltpu.make_async_copy(
            charges.at[:, pl.ds(pl.multiple_of(column, CHUNK), CHUNK)], points.at[i], load_sem.at[i])

    copies = [(rows, picks)] + [(coef.at[n], mats.at[n]) for n in range(leaves)]
    lead = len(copies)
    for b in range(m):
        index = total - (total >> early + b) + z // (1 << b + 1)
        copies.append((interp.at[index, :, pl.ds(pl.multiple_of(bit(z, b) * S, S), S)], halves.at[b]))
    where = {}
    for level in range(early, 0, -1):
        count = leaves >> level
        for k in range(count):
            where[level, k] = len(where)
            copies.append((interp.at[total - (total >> level - 1) + z * count + k], nodes.at[where[level, k]]))
    soon = len(copies)
    copies.append((top, tops))
    loads = [pltpu.make_async_copy(a, b, load_sem.at[chunks + i]) for i, (a, b) in enumerate(copies)]

    for copy in loads[:lead]:
        copy.start()
    for copy in loads[lead:soon]:
        copy.start()
    chunk_copy(0).start()

    def table_copy(delta):
        start, first, count, _ = segs[delta]
        part = pl.ds(S - (S >> first - 1), pack - S + (S >> first - 1))
        return pltpu.make_async_remote_copy(
            src_ref=top.at[part], dst_ref=tables.at[delta - 1, part], send_sem=table_send.at[delta - 1],
            recv_sem=table_recv.at[delta - 1], device_id={"leaf": flip(p, delta, L)}, device_id_type=MESH)

    def send_up(i):
        return pltpu.make_async_remote_copy(
            src_ref=parts.at[i], dst_ref=below.at[i], send_sem=up_send.at[i], recv_sem=up_recv.at[i],
            device_id={"rhs": z + 1}, device_id_type=MESH)

    def send_down(i):
        return pltpu.make_async_remote_copy(
            src_ref=parts.at[i], dst_ref=above.at[i], send_sem=down_send.at[i], recv_sem=down_recv.at[i],
            device_id={"rhs": z - 1}, device_id_type=MESH)

    def part_copy(q, delta):
        start, _, _, padded = segs[delta]
        ref = pl.ds(start, padded)
        return pltpu.make_async_remote_copy(
            src_ref=leaving.at[q, ref], dst_ref=coming.at[q, ref], send_sem=part_send.at[q, delta - 1],
            recv_sem=part_recv.at[q, delta - 1], device_id={"leaf": flip(p, delta, L)}, device_id_type=MESH)

    @pl.when(z == 0)
    def _():
        for q in range(Q):
            below[q] = jnp.zeros((S, PIECE), bf)

    @pl.when(z == R - 1)
    def _():
        for q in range(Q):
            above[(R - 1) * Q + q] = jnp.zeros((S, PIECE), bf)

    for copy in loads[:lead]:
        copy.wait()
    lanes = lax.broadcasted_iota(jnp.int32, (S, 128), 1)
    for n in range(leaves):
        across = jnp.transpose(jnp.broadcast_to(picks[n:n + 1, :], (128, S)))
        for t in range(M // 128):
            part = slice(t * 128, (t + 1) * 128)
            mats[n, :, part] = (mats[n, :, part].astype(jnp.float32)
                                + jnp.where(across == lanes + t * 128, 1.0, 0.0)).astype(bf)
    for i in range(1, chunks):
        chunk_copy(i).start()
    loads[-1].start()
    pl.semaphore_wait(barrier, neighbours + n_leaf - 1)
    for delta in range(1, n_leaf):
        table_copy(delta).start()
    for copy in loads[lead:soon]:
        copy.wait()

    def leaf_stage(i):
        chunk_copy(i).wait()
        for n in range(leaves):
            leafw[n * S:(n + 1) * S, :] = dot(mats[n], points[i, n * M:(n + 1) * M, :]).astype(bf)

    def compose():
        op = None
        for b in range(m):
            if b == 0:
                op = halves[0]
            else:
                op = dot(halves[b], op).astype(bf)
        current = [op]
        for level in range(early, 0, -1):
            following = []
            for k in range(leaves >> level):
                matrix = nodes[where[level, k]]
                value = matrix if current[k] is None else dot(current[k], matrix).astype(bf)
                if level == 1:
                    skel[:, 2 * k * S:(2 * k + 2) * S] = value
                else:
                    ops[where[level, k]] = value
                    following += [ops[where[level, k], :, :S], ops[where[level, k], :, S:]]
            current = following
        if early == 0:
            rows_at = lax.broadcasted_iota(jnp.int32, (S, S), 0)
            same = jnp.where(rows_at == lax.broadcasted_iota(jnp.int32, (S, S), 1), 1.0, 0.0).astype(bf)
            skel[...] = same if op is None else op

    def chunk(i):
        leaf_stage(i)
        if i == 0:
            compose()
        value = dot(skel[...], leafw[...]).astype(bf)
        c = block(i // H)
        base = c * Q + i % H * (CHUNK // PIECE)
        for j in range(CHUNK // PIECE):
            parts[base + j] = value[:, j * PIECE:(j + 1) * PIECE]
        if i < chunks - H and R > 1:
            @pl.when(z == 0)
            def _():
                for j in range(CHUNK // PIECE):
                    send_up(base + j).start()

            @pl.when(z == R - 1)
            def _():
                for j in range(CHUNK // PIECE):
                    send_down(base + j).start()

    def prepare_top():
        loads[-1].wait()
        for delta in range(1, n_leaf):
            table_copy(delta).wait_recv()
        for level in range(1, L + 1):
            offset, count = S - (S >> level - 1), S >> level
            half = pl.ds(pl.multiple_of(bit(p, level - 1) * S, S), S)
            for delta in range(1 << level):
                source = tops if delta == 0 else tables.at[delta - 1]
                rows_of = source[offset:offset + count, half]
                if level == 1:
                    put_top(level, delta, rows_of)
                else:
                    level_ops[1, delta * count:(delta + 1) * count, :] = rows_of
            if level > 1:
                value = dot(level_ops[1], level_ops[0]).astype(bf)
                for delta in range(1 << level):
                    put_top(level, delta, value[delta * count:(delta + 1) * count])

    def put_top(level, delta, value):
        start, first, _, _ = segs[delta]
        offset, count = (S >> first - 1) - (S >> level - 1), S >> level
        wide[start + offset:start + offset + count, :] = value
        if level < L:
            place = flip(p, delta, L) % (1 << level)
            level_ops[0, pl.ds(pl.multiple_of(place * count, count), count), :] = value

    def add_into(i, other):
        parts[i] = (parts[i].astype(jnp.float32) + other[i].astype(jnp.float32)).astype(bf)

    def any_device(test):
        return any(test(k) for k in range(R))

    def step(t):
        if any_device(lambda k: k > 0 and 0 <= t - LAG * k < (R - 1 - k) * Q):
            s = t - LAG * z

            @pl.when((z > 0) & (s >= 0) & (s < (R - 1 - z) * Q))
            def _():
                i = (R - 1 - s // Q) * Q + s % Q
                send_up(i).wait_recv()
                add_into(i, below)
                send_up(i).start()

        if any_device(lambda k: k < R - 1 and 0 <= t - LAG * (R - 1 - k) < k * Q):
            s_down = t - LAG * (R - 1 - z)

            @pl.when((z < R - 1) & (s_down >= 0) & (s_down < z * Q))
            def _():
                send_down(s_down).wait_recv()
                add_into(s_down, above)
                send_down(s_down).start()

        finals = [final_step(R, Q, k) for k in range(R)]
        if any_device(lambda k: 0 <= t - finals[k] < Q):
            q = t - chosen(z, finals)

            @pl.when((q >= 0) & (q < Q))
            def _():
                finish(q)

    def finish(q):
        i = z * Q + q
        if R > 1:
            @pl.when(z > 0)
            def _():
                send_up(i).wait_recv()

            @pl.when(z < R - 1)
            def _():
                send_down(i).wait_recv()
        root = (parts[i].astype(jnp.float32) + below[i].astype(jnp.float32)
                + above[i].astype(jnp.float32)).astype(bf)
        root_out[:, pl.ds(pl.multiple_of(q * PIECE, PIECE), PIECE)] = root
        leaving[q] = dot(wide[...], root).astype(bf)
        for delta in range(1, n_leaf):
            part_copy(q, delta).start()

    steps = max(final_step(R, Q, k) for k in range(R)) + Q
    needed = []
    for t in range(steps):
        need = 0
        for k in range(R):
            s, s_down = t - LAG * k, t - LAG * (R - 1 - k)
            blocks = []
            if k > 0 and 0 <= s < (R - 1 - k) * Q:
                blocks.append((R - 1 - s // Q, s % Q))
            if k < R - 1 and 0 <= s_down < k * Q:
                blocks.append((s_down // Q, s_down % Q))
            if 0 <= t - final_step(R, Q, k) < Q:
                blocks.append((k, t - final_step(R, Q, k)))
            for c, q in blocks:
                need = max(need, orders[k].index(c) * H + q // (CHUNK // PIECE) + 1)
        needed.append(need)
    earliest = min(final_step(R, Q, k) for k in range(R))

    made = 0
    prepared = False
    for t in range(steps):
        while made < chunks and (made < needed[t] or made < min(t + AHEAD, chunks)):
            chunk(made)
            made += 1
        if made == chunks and not prepared or t == earliest and not prepared:
            prepare_top()
            prepared = True
        step(t)

    for q in range(Q):
        for delta in range(1, n_leaf):
            part_copy(q, delta).wait_recv()
        for level in range(1, L + 1):
            offset, count = S - (S >> level - 1), S >> level
            value = None
            for delta in range(1 << level):
                start, first, _, _ = segs[delta]
                at = start + (S >> first - 1) - (S >> level - 1)
                source = leaving if delta == 0 else coming
                term = source[q, at:at + count, :].astype(jnp.float32)
                value = term if value is None else value + term
            top_out[offset:offset + count, q * PIECE:(q + 1) * PIECE] = value.astype(bf)

    for delta in range(1, n_leaf):
        table_copy(delta).wait_send()
        for q in range(Q):
            part_copy(q, delta).wait_send()
    if R > 1:
        for i in range(R * Q):
            @pl.when((z < R - 1) & (z < i // Q))
            def _():
                send_up(i).wait_send()

            @pl.when((z > 0) & (z > i // Q))
            def _():
                send_down(i).wait_send()


def store(root, top, root_out, top_out, sems):
    copies = [pltpu.make_async_copy(root, root_out, sems.at[0]),
              pltpu.make_async_copy(top, top_out, sems.at[1])]
    for copy in copies:
        copy.start()
    for copy in copies:
        copy.wait()


def local(charges, leaf_coef, leaf_rows, local_interp, top_interp):
    R, n_leaf = lax.axis_size("rhs"), lax.axis_size("leaf")
    leaves, S, M = leaf_coef.shape
    cols = charges.shape[1]
    m, L = R.bit_length() - 1, n_leaf.bit_length() - 1
    early = leaves.bit_length() - 1
    width = cols // R
    H, Q = width // CHUNK, width // PIECE
    plan = dict(R=R, L=L, H=H, Q=Q, leaves=leaves, S=S, M=M, m=m, n_leaf=n_leaf, early=early)
    bf = jnp.bfloat16
    pack = top_interp.shape[0]
    _, height = segments(S, L, n_leaf)
    any_spec = pl.BlockSpec(memory_space=pl.ANY)
    vmem = pl.BlockSpec(memory_space=pltpu.VMEM)
    node_count = max(leaves - 1, 1)
    peers = max(n_leaf - 1, 1)
    dma = pltpu.SemaphoreType.DMA
    results = pl.pallas_call(
        functools.partial(kernel, plan),
        out_shape=(jax.ShapeDtypeStruct((S, width), bf), jax.ShapeDtypeStruct((pack, width), bf)),
        in_specs=[any_spec] * 5,
        out_specs=(vmem, vmem),
        scratch_shapes=[
            pltpu.VMEM((R * H, leaves * M, CHUNK), bf),
            pltpu.VMEM((leaves, S, M), bf),
            pltpu.VMEM((leaves, S), jnp.int32),
            pltpu.VMEM((node_count, S, 2 * S), bf),
            pltpu.VMEM((max(m, 1), S, S), bf),
            pltpu.VMEM((node_count, S, 2 * S), bf),
            pltpu.VMEM((S, leaves * S), bf),
            pltpu.VMEM((leaves * S, CHUNK), bf),
            pltpu.VMEM((pack, 2 * S), bf),
            pltpu.VMEM((peers, pack, 2 * S), bf),
            pltpu.VMEM((height, S), bf),
            pltpu.VMEM((2, S, S), bf),
            pltpu.VMEM((R * Q, S, PIECE), bf),
            pltpu.VMEM((R * Q, S, PIECE), bf),
            pltpu.VMEM((R * Q, S, PIECE), bf),
            pltpu.VMEM((Q, height, PIECE), bf),
            pltpu.VMEM((Q, height, PIECE), bf),
            dma((R * H + 2 + leaves + node_count + m,)),
            dma((R * Q,)),
            dma((R * Q,)),
            dma((R * Q,)),
            dma((R * Q,)),
            dma((peers,)),
            dma((peers,)),
            dma((Q, peers)),
            dma((Q, peers)),
        ],
        compiler_params=pltpu.CompilerParams(collective_id=0, has_side_effects=True,
                                             vmem_limit_bytes=60 * 1024 * 1024),
    )(charges, leaf_coef, leaf_rows, local_interp, top_interp)
    return pl.pallas_call(
        store,
        out_shape=(jax.ShapeDtypeStruct((S, width), bf), jax.ShapeDtypeStruct((pack, width), bf)),
        in_specs=[vmem, vmem],
        out_specs=(any_spec, any_spec),
        scratch_shapes=[pltpu.SemaphoreType.DMA((2,))],
    )(*results)


def solution(mesh):
    placed = (
        P(("leaf", "rhs"), None),
        P(("leaf", "rhs"), None, None),
        P(("leaf", "rhs"), None),
        P("leaf", None, None),
        P("leaf", None),
    )
    return jax.shard_map(
        local,
        mesh=mesh,
        in_specs=placed,
        out_specs=(P("leaf", "rhs"), P("leaf", "rhs")),
        check_vma=False,
    )
```

```python
import functools

import jax
import jax.numpy as jnp
from jax import lax
from jax.experimental import pallas as pl
from jax.experimental.pallas import tpu as pltpu
from jax.sharding import PartitionSpec as P

PIECE = 128
CHUNK = 256
LAG = 2
AHEAD = 5
EARLY = 1
TABLES = 2
WAIT = 3
MESH = pl.DeviceIdType.MESH


def bit(value, k):
    return (value // (1 << k)) % 2


def flip(value, offset, bits):
    out = 0
    for k in range(bits):
        a, b = bit(value, k), bit(offset, k)
        out = out + (a + b - 2 * a * b) * (1 << k)
    return out


def chosen(z, table):
    size = len(table)
    if len(set(table)) == 1:
        return table[0]
    out = 0
    for k, value in enumerate(table):
        differs = ((z - k + size) % size + size - 1) // size
        out = out + (1 - differs) * value
    return out


def dot(a, b):
    return jnp.dot(a, b, preferred_element_type=jnp.float32)


def up_block(R, i):
    return R - 1 - i


def block_order(R, Q, z):
    when = {}
    for c in range(R):
        if c > z:
            when[c] = LAG * z + (R - 1 - c) * Q
        elif c < z:
            when[c] = LAG * (R - 1 - z) + c * Q
        else:
            when[c] = final_step(R, Q, z)
    first = (lambda c: -c) if z < R / 2 else (lambda c: c)
    return sorted(range(R), key=lambda c: (c == z, when[c], first(c)))


def final_step(R, Q, z):
    below = LAG * z + (R - 1 - z) * Q if z > 0 else 0
    above = LAG * (R - 1 - z) + z * Q if z < R - 1 else 0
    return max(below, above)


def segments(S, L, n_leaf):
    out, start = [], 0
    for delta in range(n_leaf):
        first = max(delta.bit_length(), 1)
        rows = (S >> first - 1) - (S >> L)
        padded = -(-rows // 32) * 32
        out.append((start, first, rows, padded))
        start += padded
    return out, start


def kernel(plan, charges, coef, rows, interp, top, root_out, top_out, *scratch):
    (points, mats, picks, nodes, halves, ops, skel, leafw, tops, tables, wide, level_ops, parts,
     below, above, leaving, coming, sums, extra, load_sem, up_send, up_recv, down_send, down_recv,
     table_send, table_recv, part_send, part_recv, sum_send, sum_recv) = scratch
    R, L, H, Q = plan["R"], plan["L"], plan["H"], plan["Q"]
    leaves, S, M = plan["leaves"], plan["S"], plan["M"]
    m, n_leaf, early = plan["m"], plan["n_leaf"], plan["early"]
    pack = top.shape[0]
    total = leaves * R
    bf = jnp.bfloat16
    z = lax.axis_index("rhs")
    p = lax.axis_index("leaf")
    segs, height = segments(S, L, n_leaf)
    orders = [block_order(R, Q, k) for k in range(R)]
    chunks = R * H
    hurried = EARLY if R > 1 else 0
    earliest = min(final_step(R, Q, k) for k in range(R))

    barrier = pltpu.get_barrier_semaphore()
    if R > 1:
        @pl.when(z > 0)
        def _():
            pl.semaphore_signal(barrier, inc=1, device_id={"rhs": z - 1}, device_id_type=MESH)

        @pl.when(z < R - 1)
        def _():
            pl.semaphore_signal(barrier, inc=1, device_id={"rhs": z + 1}, device_id_type=MESH)
    for b in range(L):
        pl.semaphore_signal(barrier, inc=1, device_id={"leaf": flip(p, 1 << b, L)}, device_id_type=MESH)
    neighbours = chosen(z, [(k > 0) + (k < R - 1) for k in range(R)])

    def block(i):
        return chosen(z, [orders[k][i] for k in range(R)])

    def chunk_copy(i):
        column = (block(i // H) * H + i % H) * CHUNK
        return pltpu.make_async_copy(
            charges.at[:, pl.ds(pl.multiple_of(column, CHUNK), CHUNK)], points.at[i], load_sem.at[i])

    copies = [(rows, picks)] + [(coef.at[n], mats.at[n]) for n in range(leaves)]
    lead = len(copies)
    for b in range(m):
        index = total - (total >> early + b) + z // (1 << b + 1)
        copies.append((interp.at[index, :, pl.ds(pl.multiple_of(bit(z, b) * S, S), S)], halves.at[b]))
    where = {}
    for level in range(early, 0, -1):
        count = leaves >> level
        for k in range(count):
            where[level, k] = len(where)
            copies.append((interp.at[total - (total >> level - 1) + z * count + k], nodes.at[where[level, k]]))
    copies.append((top, tops))
    soon = len(copies)
    loads = [pltpu.make_async_copy(a, b, load_sem.at[chunks + i]) for i, (a, b) in enumerate(copies)]

    for copy in loads[:lead]:
        copy.start()
    for copy in loads[lead:soon]:
        copy.start()
    chunk_copy(0).start()

    def table_copies(delta):
        peer = flip(p, delta, L)
        out = []
        for level in range(segs[delta][1], L + 1):
            part = pl.ds(S - (S >> level - 1), S >> level)
            half = pl.ds(pl.multiple_of(bit(peer, level - 1) * S, S), S)
            out.append(pltpu.make_async_remote_copy(
                src_ref=tops.at[part, half], dst_ref=tables.at[delta - 1, part],
                send_sem=table_send.at[delta - 1, level - 1], recv_sem=table_recv.at[delta - 1, level - 1],
                device_id={"leaf": peer}, device_id_type=MESH))
        return out

    stages = [[d for d in range(1, n_leaf) if bin(d).count("1") == k] for k in range(L + 1)]

    def table_stage(k):
        if k > 1:
            for delta in stages[k - 1]:
                for copy in table_copies(delta):
                    copy.wait_recv()
        if k <= L:
            for delta in stages[k]:
                for copy in table_copies(delta):
                    copy.start()

    def send_up(i):
        return pltpu.make_async_remote_copy(
            src_ref=parts.at[i], dst_ref=below.at[i], send_sem=up_send.at[i], recv_sem=up_recv.at[i],
            device_id={"rhs": z + 1}, device_id_type=MESH)

    def send_down(i):
        return pltpu.make_async_remote_copy(
            src_ref=parts.at[i], dst_ref=above.at[i], send_sem=down_send.at[i], recv_sem=down_recv.at[i],
            device_id={"rhs": z - 1}, device_id_type=MESH)

    def part_copy(q, delta):
        start, _, _, padded = segs[delta]
        ref = pl.ds(start, padded)
        return pltpu.make_async_remote_copy(
            src_ref=leaving.at[q, ref], dst_ref=coming.at[q, ref], send_sem=part_send.at[q, delta - 1],
            recv_sem=part_recv.at[q, delta - 1], device_id={"leaf": flip(p, delta, L)}, device_id_type=MESH)

    if hurried:
        @pl.when(chosen(z, [int(k in (1, R - 2)) for k in range(R)]) == 0)
        def _():
            extra[...] = jnp.zeros_like(extra)

    @pl.when(z == 0)
    def _():
        for q in range(Q):
            below[q] = jnp.zeros((S, PIECE), bf)

    @pl.when(z == R - 1)
    def _():
        for q in range(Q):
            above[(R - 1) * Q + q] = jnp.zeros((S, PIECE), bf)

    for copy in loads[:lead]:
        copy.wait()
    lanes = lax.broadcasted_iota(jnp.int32, (S, 128), 1)
    for n in range(leaves):
        across = jnp.transpose(jnp.broadcast_to(picks[n:n + 1, :], (128, S)))
        for t in range(M // 128):
            part = slice(t * 128, (t + 1) * 128)
            mats[n, :, part] = (mats[n, :, part].astype(jnp.float32)
                                + jnp.where(across == lanes + t * 128, 1.0, 0.0)).astype(bf)
    for i in range(1, chunks):
        chunk_copy(i).start()
    for copy in loads[lead:soon]:
        copy.wait()

    def leaf_stage(i):
        chunk_copy(i).wait()
        for n in range(leaves):
            leafw[n * S:(n + 1) * S, :] = dot(mats[n], points[i, n * M:(n + 1) * M, :]).astype(bf)

    def compose():
        op = None
        for b in range(m):
            if b == 0:
                op = halves[0]
            else:
                op = dot(halves[b], op).astype(bf)
        current = [op]
        for level in range(early, 0, -1):
            following = []
            for k in range(leaves >> level):
                matrix = nodes[where[level, k]]
                value = matrix if current[k] is None else dot(current[k], matrix).astype(bf)
                if level == 1:
                    skel[:, 2 * k * S:(2 * k + 2) * S] = value
                else:
                    ops[where[level, k]] = value
                    following += [ops[where[level, k], :, :S], ops[where[level, k], :, S:]]
            current = following
        if early == 0:
            rows_at = lax.broadcasted_iota(jnp.int32, (S, S), 0)
            same = jnp.where(rows_at == lax.broadcasted_iota(jnp.int32, (S, S), 1), 1.0, 0.0).astype(bf)
            skel[...] = same if op is None else op

    def chunk(i):
        leaf_stage(i)
        if i == 0:
            compose()
        value = dot(skel[...], leafw[...]).astype(bf)
        c = block(i // H)
        base = c * Q + i % H * (CHUNK // PIECE)
        for j in range(CHUNK // PIECE):
            parts[base + j] = value[:, j * PIECE:(j + 1) * PIECE]
        if i == 0:
            pl.semaphore_wait(barrier, neighbours + L)
            table_stage(1)
        if i < chunks - H and R > 1:
            @pl.when(z == 0)
            def _():
                for j in range(CHUNK // PIECE):
                    send_up(base + j).start()

            @pl.when(z == R - 1)
            def _():
                for j in range(CHUNK // PIECE):
                    send_down(base + j).start()

    def prepare_top():
        for level in range(1, L + 1):
            offset, count = S - (S >> level - 1), S >> level
            half = pl.ds(pl.multiple_of(bit(p, level - 1) * S, S), S)
            for delta in range(1 << level):
                if delta == 0:
                    rows_of = tops[offset:offset + count, half]
                else:
                    rows_of = tables[delta - 1, offset:offset + count, :]
                if level == 1:
                    put_top(level, delta, rows_of)
                else:
                    level_ops[1, delta * count:(delta + 1) * count, :] = rows_of
            if level > 1:
                value = dot(level_ops[1], level_ops[0]).astype(bf)
                for delta in range(1 << level):
                    put_top(level, delta, value[delta * count:(delta + 1) * count])

    def put_top(level, delta, value):
        start, first, _, _ = segs[delta]
        offset, count = (S >> first - 1) - (S >> level - 1), S >> level
        wide[start + offset:start + offset + count, :] = value
        if level < L:
            place = flip(p, delta, L) % (1 << level)
            level_ops[0, pl.ds(pl.multiple_of(place * count, count), count), :] = value

    def add_into(i, other):
        parts[i] = (parts[i].astype(jnp.float32) + other[i].astype(jnp.float32)).astype(bf)

    def any_device(test):
        return any(test(k) for k in range(R))

    def step(t):
        if any_device(lambda k: k > 0 and 0 <= t - LAG * k < (R - 1 - k) * Q):
            s = t - LAG * z

            @pl.when((z > 0) & (s >= 0) & (s < (R - 1 - z) * Q))
            def _():
                i = (R - 1 - s // Q) * Q + s % Q
                send_up(i).wait_recv()
                add_into(i, below)
                send_up(i).start()

        if any_device(lambda k: k < R - 1 and 0 <= t - LAG * (R - 1 - k) < k * Q):
            s_down = t - LAG * (R - 1 - z)

            @pl.when((z < R - 1) & (s_down >= 0) & (s_down < z * Q))
            def _():
                send_down(s_down).wait_recv()
                add_into(s_down, above)
                send_down(s_down).start()

        for j in range(hurried):
            q = Q - hurried + j
            if any_device(lambda k: late(k) and t == hurry_step(k, q)):
                now = chosen(z, [late(k) * (t == hurry_step(k, q)) for k in range(R)])

                @pl.when(now == 1)
                def _():
                    hurry(q)

        finals = [final_step(R, Q, k) for k in range(R)]
        if any_device(lambda k: 0 <= t - finals[k] < Q):
            q = t - chosen(z, finals)
            last = chosen(z, [Q - hurried * late(k) for k in range(R)])

            @pl.when((q >= 0) & (q < last))
            def _():
                finish(q)

    def finish(q):
        i = z * Q + q
        if R > 1:
            @pl.when(z > 0)
            def _():
                send_up(i).wait_recv()

            @pl.when(z < R - 1)
            def _():
                send_down(i).wait_recv()
        root = (parts[i].astype(jnp.float32) + below[i].astype(jnp.float32)
                + above[i].astype(jnp.float32)).astype(bf)
        root_out[:, pl.ds(pl.multiple_of(q * PIECE, PIECE), PIECE)] = root
        spread(q, root)

    def spread(q, value):
        leaving[q] = dot(wide[...], value).astype(bf)
        for delta in range(1, n_leaf):
            part_copy(q, delta).start()

    def late(k):
        return int(R > 1 and k in (1, R - 2))

    def hurry_step(k, q):
        other = LAG * (R - 1 - k) + k * Q if k == 1 else LAG * k + (R - 1 - k) * Q
        return max((other if R > 2 else 0) + q, earliest)

    def hurry(q):
        i = z * Q + q

        @pl.when(z == 1)
        def _():
            if R > 2:
                send_down(i).wait_recv()
            add_into(i, above)

        @pl.when(z == R - 2)
        def _():
            if R > 2:
                send_up(i).wait_recv()
            add_into(i, below)

        spread(q, parts[i])

    def sum_copy(j, upward):
        return pltpu.make_async_remote_copy(
            src_ref=sums.at[j], dst_ref=extra.at[j], send_sem=sum_send.at[j], recv_sem=sum_recv.at[j],
            device_id={"rhs": z + 1 if upward else z - 1}, device_id_type=MESH)

    def gather(q):
        for delta in range(1, n_leaf):
            part_copy(q, delta).wait_recv()
        out = []
        for level in range(1, L + 1):
            offset, count = S - (S >> level - 1), S >> level
            value = None
            for delta in range(1 << level):
                start, first, _, _ = segs[delta]
                at = start + (S >> first - 1) - (S >> level - 1)
                source = leaving if delta == 0 else coming
                term = source[q, at:at + count, :].astype(jnp.float32)
                value = term if value is None else value + term
            out.append((offset, count, value))
        return out

    def end_begin():
        @pl.when((z == 0) | (z == R - 1))
        def _():
            target = chosen(z, [1 if k == 0 else R - 2 for k in range(R)])
            for j in range(hurried):
                spread(Q + j, parts[target * Q + Q - hurried + j])

    def end_finish():
        @pl.when((z == 0) | (z == R - 1))
        def _():
            for j in range(hurried):
                for offset, count, value in gather(Q + j):
                    sums[j, offset:offset + count, :] = value.astype(bf)

        @pl.when(z == 0)
        def _():
            for j in range(hurried):
                sum_copy(j, True).start()

        @pl.when(z == R - 1)
        def _():
            for j in range(hurried):
                sum_copy(j, False).start()

    steps = max(final_step(R, Q, k) for k in range(R)) + Q
    needed = []
    for t in range(steps):
        need = 0
        for k in range(R):
            s, s_down = t - LAG * k, t - LAG * (R - 1 - k)
            blocks = []
            if k > 0 and 0 <= s < (R - 1 - k) * Q:
                blocks.append((R - 1 - s // Q, s % Q))
            if k < R - 1 and 0 <= s_down < k * Q:
                blocks.append((s_down // Q, s_down % Q))
            if 0 <= t - final_step(R, Q, k) < Q:
                blocks.append((k, t - final_step(R, Q, k)))
            for c, q in blocks:
                need = max(need, orders[k].index(c) * H + q // (CHUNK // PIECE) + 1)
        for j in range(hurried):
            q = Q - hurried + j
            for k in range(R):
                if late(k) and t == hurry_step(k, q):
                    need = max(need, orders[k].index(k) * H + q // (CHUNK // PIECE) + 1)
        if t >= earliest:
            need = max(need, chunks if hurried else 0)
        needed.append(need)

    made, stage = 0, 2
    for t in range(steps):
        while made < chunks and (made < needed[t] or made < min(t + AHEAD, chunks)):
            chunk(made)
            made += 1
            if made == AHEAD and stage == 2:
                table_stage(stage)
                stage += 1
        if made == chunks and stage <= L and t < earliest and t >= TABLES * (stage - 1):
            table_stage(stage)
            stage += 1
        if t == earliest:
            while stage <= L + 1:
                table_stage(stage)
                stage += 1
            prepare_top()
            if hurried:
                end_begin()
        if hurried and t == earliest + WAIT:
            end_finish()
        step(t)

    for q in range(Q):
        j = q - (Q - hurried)
        columns = slice(q * PIECE, (q + 1) * PIECE)
        values = gather(q)
        if j >= 0:
            i = z * Q + q

            @pl.when(z == 1)
            def _():
                send_up(i).wait_recv()
                root_out[:, columns] = (parts[i].astype(jnp.float32) + below[i].astype(jnp.float32)).astype(bf)
                sum_copy(j, True).wait_recv()

            @pl.when(z == R - 2)
            def _():
                send_down(i).wait_recv()
                root_out[:, columns] = (parts[i].astype(jnp.float32) + above[i].astype(jnp.float32)).astype(bf)
                sum_copy(j, False).wait_recv()
        for offset, count, value in values:
            if j >= 0:
                value = value + extra[j, offset:offset + count, :].astype(jnp.float32)
            top_out[offset:offset + count, columns] = value.astype(bf)

    for delta in range(1, n_leaf):
        for copy in table_copies(delta):
            copy.wait_send()
        for q in range(Q):
            part_copy(q, delta).wait_send()
    if hurried:
        @pl.when((z == 0) | (z == R - 1))
        def _():
            for j in range(hurried):
                for delta in range(1, n_leaf):
                    part_copy(Q + j, delta).wait_send()

        @pl.when(z == 0)
        def _():
            for j in range(hurried):
                sum_copy(j, True).wait_send()

        @pl.when(z == R - 1)
        def _():
            for j in range(hurried):
                sum_copy(j, False).wait_send()
    if R > 1:
        for i in range(R * Q):
            @pl.when((z < R - 1) & (z < i // Q))
            def _():
                send_up(i).wait_send()

            @pl.when((z > 0) & (z > i // Q))
            def _():
                send_down(i).wait_send()


def store(root, top, root_out, top_out, sems):
    copies = [pltpu.make_async_copy(root, root_out, sems.at[0]),
              pltpu.make_async_copy(top, top_out, sems.at[1])]
    for copy in copies:
        copy.start()
    for copy in copies:
        copy.wait()


def local(charges, leaf_coef, leaf_rows, local_interp, top_interp):
    R, n_leaf = lax.axis_size("rhs"), lax.axis_size("leaf")
    leaves, S, M = leaf_coef.shape
    cols = charges.shape[1]
    m, L = R.bit_length() - 1, n_leaf.bit_length() - 1
    early = leaves.bit_length() - 1
    width = cols // R
    H, Q = width // CHUNK, width // PIECE
    plan = dict(R=R, L=L, H=H, Q=Q, leaves=leaves, S=S, M=M, m=m, n_leaf=n_leaf, early=early)
    bf = jnp.bfloat16
    pack = top_interp.shape[0]
    _, height = segments(S, L, n_leaf)
    any_spec = pl.BlockSpec(memory_space=pl.ANY)
    vmem = pl.BlockSpec(memory_space=pltpu.VMEM)
    node_count = max(leaves - 1, 1)
    peers = max(n_leaf - 1, 1)
    dma = pltpu.SemaphoreType.DMA
    results = pl.pallas_call(
        functools.partial(kernel, plan),
        out_shape=(jax.ShapeDtypeStruct((S, width), bf), jax.ShapeDtypeStruct((pack, width), bf)),
        in_specs=[any_spec] * 5,
        out_specs=(vmem, vmem),
        scratch_shapes=[
            pltpu.VMEM((R * H, leaves * M, CHUNK), bf),
            pltpu.VMEM((leaves, S, M), bf),
            pltpu.VMEM((leaves, S), jnp.int32),
            pltpu.VMEM((node_count, S, 2 * S), bf),
            pltpu.VMEM((max(m, 1), S, S), bf),
            pltpu.VMEM((node_count, S, 2 * S), bf),
            pltpu.VMEM((S, leaves * S), bf),
            pltpu.VMEM((leaves * S, CHUNK), bf),
            pltpu.VMEM((pack, 2 * S), bf),
            pltpu.VMEM((peers, pack, S), bf),
            pltpu.VMEM((height, S), bf),
            pltpu.VMEM((2, S, S), bf),
            pltpu.VMEM((R * Q, S, PIECE), bf),
            pltpu.VMEM((R * Q, S, PIECE), bf),
            pltpu.VMEM((R * Q, S, PIECE), bf),
            pltpu.VMEM((Q + EARLY, height, PIECE), bf),
            pltpu.VMEM((Q + EARLY, height, PIECE), bf),
            pltpu.VMEM((max(EARLY, 1), pack, PIECE), bf),
            pltpu.VMEM((max(EARLY, 1), pack, PIECE), bf),
            dma((R * H + 2 + leaves + node_count + m,)),
            dma((R * Q,)),
            dma((R * Q,)),
            dma((R * Q,)),
            dma((R * Q,)),
            dma((peers, max(L, 1))),
            dma((peers, max(L, 1))),
            dma((Q + EARLY, peers)),
            dma((Q + EARLY, peers)),
            dma((max(EARLY, 1),)),
            dma((max(EARLY, 1),)),
        ],
        compiler_params=pltpu.CompilerParams(collective_id=0, has_side_effects=True,
                                             vmem_limit_bytes=60 * 1024 * 1024),
    )(charges, leaf_coef, leaf_rows, local_interp, top_interp)
    return pl.pallas_call(
        store,
        out_shape=(jax.ShapeDtypeStruct((S, width), bf), jax.ShapeDtypeStruct((pack, width), bf)),
        in_specs=[vmem, vmem],
        out_specs=(any_spec, any_spec),
        scratch_shapes=[pltpu.SemaphoreType.DMA((2,))],
    )(*results)


def solution(mesh):
    placed = (
        P(("leaf", "rhs"), None),
        P(("leaf", "rhs"), None, None),
        P(("leaf", "rhs"), None),
        P("leaf", None, None),
        P("leaf", None),
    )
    return jax.shard_map(
        local,
        mesh=mesh,
        in_specs=placed,
        out_specs=(P("leaf", "rhs"), P("leaf", "rhs")),
        check_vma=False,
    )
```

```python
import functools

import jax
import jax.numpy as jnp
from jax import lax
from jax.experimental import pallas as pl
from jax.experimental.pallas import tpu as pltpu
from jax.sharding import PartitionSpec as P

PIECE = 128
CHUNK = 256
LAG = 2
AHEAD = 5
EARLY = 0
TABLES = 2
WAIT = 3
MESH = pl.DeviceIdType.MESH


def bit(value, k):
    return (value // (1 << k)) % 2


def flip(value, offset, bits):
    out = 0
    for k in range(bits):
        a, b = bit(value, k), bit(offset, k)
        out = out + (a + b - 2 * a * b) * (1 << k)
    return out


def chosen(z, table):
    size = len(table)
    if len(set(table)) == 1:
        return table[0]
    out = 0
    for k, value in enumerate(table):
        differs = ((z - k + size) % size + size - 1) // size
        out = out + (1 - differs) * value
    return out


def dot(a, b):
    return jnp.dot(a, b, preferred_element_type=jnp.float32)


def up_block(R, i):
    return R - 1 - i


def block_order(R, Q, z):
    when = {}
    for c in range(R):
        if c > z:
            when[c] = LAG * z + (R - 1 - c) * Q
        elif c < z:
            when[c] = LAG * (R - 1 - z) + c * Q
        else:
            when[c] = final_step(R, Q, z)
    first = (lambda c: -c) if z < R / 2 else (lambda c: c)
    return sorted(range(R), key=lambda c: (c == z, when[c], first(c)))


def final_step(R, Q, z):
    below = LAG * z + (R - 1 - z) * Q if z > 0 else 0
    above = LAG * (R - 1 - z) + z * Q if z < R - 1 else 0
    return max(below, above)


def segments(S, L, n_leaf):
    out, start = [], 0
    for delta in range(n_leaf):
        first = max(delta.bit_length(), 1)
        rows = (S >> first - 1) - (S >> L)
        padded = -(-rows // 32) * 32
        out.append((start, first, rows, padded))
        start += padded
    return out, start


def kernel(plan, charges, coef, rows, interp, top, root_out, top_out, *scratch):
    (points, mats, picks, nodes, halves, ops, skel, leafw, tops, tables, wide, level_ops, parts,
     below, above, leaving, coming, sums, extra, load_sem, up_send, up_recv, down_send, down_recv,
     table_send, table_recv, part_send, part_recv, sum_send, sum_recv, hello) = scratch
    R, L, H, Q = plan["R"], plan["L"], plan["H"], plan["Q"]
    leaves, S, M = plan["leaves"], plan["S"], plan["M"]
    m, n_leaf, early = plan["m"], plan["n_leaf"], plan["early"]
    pack = top.shape[0]
    total = leaves * R
    bf = jnp.bfloat16
    z = lax.axis_index("rhs")
    p = lax.axis_index("leaf")
    segs, height = segments(S, L, n_leaf)
    orders = [block_order(R, Q, k) for k in range(R)]
    chunks = R * H
    hurried = EARLY if R > 1 else 0
    earliest = min(final_step(R, Q, k) for k in range(R))

    barrier = pltpu.get_barrier_semaphore()
    if R > 1:
        @pl.when(z > 0)
        def _():
            pl.semaphore_signal(barrier, inc=1, device_id={"rhs": z - 1}, device_id_type=MESH)

        @pl.when(z < R - 1)
        def _():
            pl.semaphore_signal(barrier, inc=1, device_id={"rhs": z + 1}, device_id_type=MESH)
    for b in range(L):
        pl.semaphore_signal(barrier, inc=1, device_id={"leaf": flip(p, 1 << b, L)}, device_id_type=MESH)
    neighbours = chosen(z, [(k > 0) + (k < R - 1) for k in range(R)])

    def block(i):
        return chosen(z, [orders[k][i] for k in range(R)])

    def chunk_copy(i):
        column = (block(i // H) * H + i % H) * CHUNK
        return pltpu.make_async_copy(
            charges.at[:, pl.ds(pl.multiple_of(column, CHUNK), CHUNK)], points.at[i], load_sem.at[i])

    copies = [(rows, picks)] + [(coef.at[n], mats.at[n]) for n in range(leaves)]
    lead = len(copies)
    for b in range(m):
        index = total - (total >> early + b) + z // (1 << b + 1)
        copies.append((interp.at[index, :, pl.ds(pl.multiple_of(bit(z, b) * S, S), S)], halves.at[b]))
    where = {}
    for level in range(early, 0, -1):
        count = leaves >> level
        for k in range(count):
            where[level, k] = len(where)
            copies.append((interp.at[total - (total >> level - 1) + z * count + k], nodes.at[where[level, k]]))
    soon = len(copies)
    copies.append((top, tops))
    loads = [pltpu.make_async_copy(a, b, load_sem.at[chunks + i]) for i, (a, b) in enumerate(copies)]

    for copy in loads[:lead]:
        copy.start()
    chunk_copy(0).start()
    for copy in loads[lead:soon]:
        copy.start()

    def table_copies(delta):
        peer = flip(p, delta, L)
        out = []
        for level in range(segs[delta][1], L + 1):
            part = pl.ds(S - (S >> level - 1), S >> level)
            half = pl.ds(pl.multiple_of(bit(peer, level - 1) * S, S), S)
            out.append(pltpu.make_async_remote_copy(
                src_ref=tops.at[part, half], dst_ref=tables.at[delta - 1, part],
                send_sem=table_send.at[delta - 1, level - 1], recv_sem=table_recv.at[delta - 1, level - 1],
                device_id={"leaf": peer}, device_id_type=MESH))
        return out

    stages = [[d for d in range(1, n_leaf) if bin(d).count("1") == k] for k in range(L + 1)]

    def table_stage(k):
        if k > 1:
            pl.semaphore_wait(hello.at[k - 2], L)
        else:
            loads[-1].wait()
        if k < L:
            for b in range(L):
                pl.semaphore_signal(hello.at[k - 1], inc=1, device_id={"leaf": flip(p, 1 << b, L)},
                                    device_id_type=MESH)
        for delta in stages[k]:
            for copy in table_copies(delta):
                copy.start()

    def send_up(i):
        return pltpu.make_async_remote_copy(
            src_ref=parts.at[i], dst_ref=below.at[i], send_sem=up_send.at[i], recv_sem=up_recv.at[i],
            device_id={"rhs": z + 1}, device_id_type=MESH)

    def send_down(i):
        return pltpu.make_async_remote_copy(
            src_ref=parts.at[i], dst_ref=above.at[i], send_sem=down_send.at[i], recv_sem=down_recv.at[i],
            device_id={"rhs": z - 1}, device_id_type=MESH)

    def part_copy(q, delta):
        start, _, _, padded = segs[delta]
        ref = pl.ds(start, padded)
        return pltpu.make_async_remote_copy(
            src_ref=leaving.at[q, ref], dst_ref=coming.at[q, ref], send_sem=part_send.at[q, delta - 1],
            recv_sem=part_recv.at[q, delta - 1], device_id={"leaf": flip(p, delta, L)}, device_id_type=MESH)

    if hurried:
        @pl.when(chosen(z, [int(k in (1, R - 2)) for k in range(R)]) == 0)
        def _():
            extra[...] = jnp.zeros_like(extra)

    @pl.when(z == 0)
    def _():
        for q in range(Q):
            below[q] = jnp.zeros((S, PIECE), bf)

    @pl.when(z == R - 1)
    def _():
        for q in range(Q):
            above[(R - 1) * Q + q] = jnp.zeros((S, PIECE), bf)

    for copy in loads[:lead]:
        copy.wait()
    lanes = lax.broadcasted_iota(jnp.int32, (S, 128), 1)
    for n in range(leaves):
        across = jnp.transpose(jnp.broadcast_to(picks[n:n + 1, :], (128, S)))
        for t in range(M // 128):
            part = slice(t * 128, (t + 1) * 128)
            mats[n, :, part] = (mats[n, :, part].astype(jnp.float32)
                                + jnp.where(across == lanes + t * 128, 1.0, 0.0)).astype(bf)
    for copy in loads[lead:soon]:
        copy.wait()
    chunk_copy(0).wait()
    loads[-1].start()
    for i in range(1, chunks):
        chunk_copy(i).start()

    def leaf_stage(i):
        if i > 0:
            chunk_copy(i).wait()
        for n in range(leaves):
            leafw[n * S:(n + 1) * S, :] = dot(mats[n], points[i, n * M:(n + 1) * M, :]).astype(bf)

    def compose():
        op = None
        for b in range(m):
            if b == 0:
                op = halves[0]
            else:
                op = dot(halves[b], op).astype(bf)
        current = [op]
        for level in range(early, 0, -1):
            following = []
            for k in range(leaves >> level):
                matrix = nodes[where[level, k]]
                value = matrix if current[k] is None else dot(current[k], matrix).astype(bf)
                if level == 1:
                    skel[:, 2 * k * S:(2 * k + 2) * S] = value
                else:
                    ops[where[level, k]] = value
                    following += [ops[where[level, k], :, :S], ops[where[level, k], :, S:]]
            current = following
        if early == 0:
            rows_at = lax.broadcasted_iota(jnp.int32, (S, S), 0)
            same = jnp.where(rows_at == lax.broadcasted_iota(jnp.int32, (S, S), 1), 1.0, 0.0).astype(bf)
            skel[...] = same if op is None else op

    def chunk(i):
        leaf_stage(i)
        if i == 0:
            compose()
        value = dot(skel[...], leafw[...]).astype(bf)
        c = block(i // H)
        base = c * Q + i % H * (CHUNK // PIECE)
        for j in range(CHUNK // PIECE):
            parts[base + j] = value[:, j * PIECE:(j + 1) * PIECE]
        if i == 0:
            pl.semaphore_wait(barrier, neighbours + L)
        if i < chunks - H and R > 1:
            @pl.when(z == 0)
            def _():
                for j in range(CHUNK // PIECE):
                    send_up(base + j).start()

            @pl.when(z == R - 1)
            def _():
                for j in range(CHUNK // PIECE):
                    send_down(base + j).start()
        if i == 0:
            table_stage(1)

    def prepare_top():
        for delta in range(1, n_leaf):
            for copy in table_copies(delta):
                copy.wait_recv()
        for level in range(1, L + 1):
            offset, count = S - (S >> level - 1), S >> level
            half = pl.ds(pl.multiple_of(bit(p, level - 1) * S, S), S)
            for delta in range(1 << level):
                if delta == 0:
                    rows_of = tops[offset:offset + count, half]
                else:
                    rows_of = tables[delta - 1, offset:offset + count, :]
                if level == 1:
                    put_top(level, delta, rows_of)
                else:
                    level_ops[1, delta * count:(delta + 1) * count, :] = rows_of
            if level > 1:
                value = dot(level_ops[1], level_ops[0]).astype(bf)
                for delta in range(1 << level):
                    put_top(level, delta, value[delta * count:(delta + 1) * count])

    def put_top(level, delta, value):
        start, first, _, _ = segs[delta]
        offset, count = (S >> first - 1) - (S >> level - 1), S >> level
        wide[start + offset:start + offset + count, :] = value
        if level < L:
            place = flip(p, delta, L) % (1 << level)
            level_ops[0, pl.ds(pl.multiple_of(place * count, count), count), :] = value

    def add_into(i, other):
        parts[i] = (parts[i].astype(jnp.float32) + other[i].astype(jnp.float32)).astype(bf)

    def any_device(test):
        return any(test(k) for k in range(R))

    def step(t):
        if any_device(lambda k: k > 0 and 0 <= t - LAG * k < (R - 1 - k) * Q):
            s = t - LAG * z

            @pl.when((z > 0) & (s >= 0) & (s < (R - 1 - z) * Q))
            def _():
                i = (R - 1 - s // Q) * Q + s % Q
                send_up(i).wait_recv()
                add_into(i, below)
                send_up(i).start()

        if any_device(lambda k: k < R - 1 and 0 <= t - LAG * (R - 1 - k) < k * Q):
            s_down = t - LAG * (R - 1 - z)

            @pl.when((z < R - 1) & (s_down >= 0) & (s_down < z * Q))
            def _():
                send_down(s_down).wait_recv()
                add_into(s_down, above)
                send_down(s_down).start()

        for j in range(hurried):
            q = Q - hurried + j
            if any_device(lambda k: late(k) and t == hurry_step(k, q)):
                now = chosen(z, [late(k) * (t == hurry_step(k, q)) for k in range(R)])

                @pl.when(now == 1)
                def _():
                    hurry(q)

        finals = [final_step(R, Q, k) for k in range(R)]
        if any_device(lambda k: 0 <= t - finals[k] < Q):
            q = t - chosen(z, finals)
            last = chosen(z, [Q - hurried * late(k) for k in range(R)])

            @pl.when((q >= 0) & (q < last))
            def _():
                finish(q)

    def finish(q):
        i = z * Q + q
        if R > 1:
            @pl.when(z > 0)
            def _():
                send_up(i).wait_recv()

            @pl.when(z < R - 1)
            def _():
                send_down(i).wait_recv()
        root = (parts[i].astype(jnp.float32) + below[i].astype(jnp.float32)
                + above[i].astype(jnp.float32)).astype(bf)
        root_out[:, pl.ds(pl.multiple_of(q * PIECE, PIECE), PIECE)] = root
        spread(q, root)

    def spread(q, value):
        leaving[q] = dot(wide[...], value).astype(bf)
        for delta in range(1, n_leaf):
            part_copy(q, delta).start()

    def late(k):
        return int(R > 1 and k in (1, R - 2))

    def hurry_step(k, q):
        other = LAG * (R - 1 - k) + k * Q if k == 1 else LAG * k + (R - 1 - k) * Q
        return max((other if R > 2 else 0) + q, earliest)

    def hurry(q):
        i = z * Q + q

        @pl.when(z == 1)
        def _():
            if R > 2:
                send_down(i).wait_recv()
            add_into(i, above)

        @pl.when(z == R - 2)
        def _():
            if R > 2:
                send_up(i).wait_recv()
            add_into(i, below)

        spread(q, parts[i])

    def sum_copy(j, upward):
        return pltpu.make_async_remote_copy(
            src_ref=sums.at[j], dst_ref=extra.at[j], send_sem=sum_send.at[j], recv_sem=sum_recv.at[j],
            device_id={"rhs": z + 1 if upward else z - 1}, device_id_type=MESH)

    def gather(q):
        for delta in range(1, n_leaf):
            part_copy(q, delta).wait_recv()
        out = []
        for level in range(1, L + 1):
            offset, count = S - (S >> level - 1), S >> level
            value = None
            for delta in range(1 << level):
                start, first, _, _ = segs[delta]
                at = start + (S >> first - 1) - (S >> level - 1)
                source = leaving if delta == 0 else coming
                term = source[q, at:at + count, :].astype(jnp.float32)
                value = term if value is None else value + term
            out.append((offset, count, value))
        return out

    def end_begin():
        @pl.when((z == 0) | (z == R - 1))
        def _():
            target = chosen(z, [1 if k == 0 else R - 2 for k in range(R)])
            for j in range(hurried):
                spread(Q + j, parts[target * Q + Q - hurried + j])

    def end_finish():
        @pl.when((z == 0) | (z == R - 1))
        def _():
            for j in range(hurried):
                for offset, count, value in gather(Q + j):
                    sums[j, offset:offset + count, :] = value.astype(bf)

        @pl.when(z == 0)
        def _():
            for j in range(hurried):
                sum_copy(j, True).start()

        @pl.when(z == R - 1)
        def _():
            for j in range(hurried):
                sum_copy(j, False).start()

    steps = max(final_step(R, Q, k) for k in range(R)) + Q
    needed = []
    for t in range(steps):
        need = 0
        for k in range(R):
            s, s_down = t - LAG * k, t - LAG * (R - 1 - k)
            blocks = []
            if k > 0 and 0 <= s < (R - 1 - k) * Q:
                blocks.append((R - 1 - s // Q, s % Q))
            if k < R - 1 and 0 <= s_down < k * Q:
                blocks.append((s_down // Q, s_down % Q))
            if 0 <= t - final_step(R, Q, k) < Q:
                blocks.append((k, t - final_step(R, Q, k)))
            for c, q in blocks:
                need = max(need, orders[k].index(c) * H + q // (CHUNK // PIECE) + 1)
        for j in range(hurried):
            q = Q - hurried + j
            for k in range(R):
                if late(k) and t == hurry_step(k, q):
                    need = max(need, orders[k].index(k) * H + q // (CHUNK // PIECE) + 1)
        if t >= earliest:
            need = max(need, chunks if hurried else 0)
        needed.append(need)

    made, stage = 0, 2
    for t in range(steps):
        while made < chunks and (made < needed[t] or made < min(t + AHEAD, chunks)):
            chunk(made)
            made += 1
            if stage <= L and made >= TABLES * (stage - 1):
                table_stage(stage)
                stage += 1
        if t == earliest:
            while stage <= L:
                table_stage(stage)
                stage += 1
            prepare_top()
            if hurried:
                end_begin()
        if hurried and t == earliest + WAIT:
            end_finish()
        step(t)

    for q in range(Q):
        j = q - (Q - hurried)
        columns = slice(q * PIECE, (q + 1) * PIECE)
        values = gather(q)
        if j >= 0:
            i = z * Q + q

            @pl.when(z == 1)
            def _():
                send_up(i).wait_recv()
                root_out[:, columns] = (parts[i].astype(jnp.float32) + below[i].astype(jnp.float32)).astype(bf)
                sum_copy(j, True).wait_recv()

            @pl.when(z == R - 2)
            def _():
                send_down(i).wait_recv()
                root_out[:, columns] = (parts[i].astype(jnp.float32) + above[i].astype(jnp.float32)).astype(bf)
                sum_copy(j, False).wait_recv()
        for offset, count, value in values:
            if j >= 0:
                value = value + extra[j, offset:offset + count, :].astype(jnp.float32)
            top_out[offset:offset + count, columns] = value.astype(bf)

    for delta in range(1, n_leaf):
        for copy in table_copies(delta):
            copy.wait_send()
        for q in range(Q):
            part_copy(q, delta).wait_send()
    if hurried:
        @pl.when((z == 0) | (z == R - 1))
        def _():
            for j in range(hurried):
                for delta in range(1, n_leaf):
                    part_copy(Q + j, delta).wait_send()

        @pl.when(z == 0)
        def _():
            for j in range(hurried):
                sum_copy(j, True).wait_send()

        @pl.when(z == R - 1)
        def _():
            for j in range(hurried):
                sum_copy(j, False).wait_send()
    if R > 1:
        for i in range(R * Q):
            @pl.when((z < R - 1) & (z < i // Q))
            def _():
                send_up(i).wait_send()

            @pl.when((z > 0) & (z > i // Q))
            def _():
                send_down(i).wait_send()


def store(root, top, root_out, top_out, sems):
    copies = [pltpu.make_async_copy(root, root_out, sems.at[0]),
              pltpu.make_async_copy(top, top_out, sems.at[1])]
    for copy in copies:
        copy.start()
    for copy in copies:
        copy.wait()


def local(charges, leaf_coef, leaf_rows, local_interp, top_interp):
    R, n_leaf = lax.axis_size("rhs"), lax.axis_size("leaf")
    leaves, S, M = leaf_coef.shape
    cols = charges.shape[1]
    m, L = R.bit_length() - 1, n_leaf.bit_length() - 1
    early = leaves.bit_length() - 1
    width = cols // R
    H, Q = width // CHUNK, width // PIECE
    plan = dict(R=R, L=L, H=H, Q=Q, leaves=leaves, S=S, M=M, m=m, n_leaf=n_leaf, early=early)
    bf = jnp.bfloat16
    pack = top_interp.shape[0]
    _, height = segments(S, L, n_leaf)
    any_spec = pl.BlockSpec(memory_space=pl.ANY)
    vmem = pl.BlockSpec(memory_space=pltpu.VMEM)
    node_count = max(leaves - 1, 1)
    peers = max(n_leaf - 1, 1)
    dma = pltpu.SemaphoreType.DMA
    results = pl.pallas_call(
        functools.partial(kernel, plan),
        out_shape=(pltpu.VMEM((S, width), bf), pltpu.VMEM((pack, width), bf)),
        in_specs=[pl.BlockSpec(memory_space=pltpu.HBM)] * 5,
        out_specs=(vmem, vmem),
        scratch_shapes=[
            pltpu.VMEM((R * H, leaves * M, CHUNK), bf),
            pltpu.VMEM((leaves, S, M), bf),
            pltpu.VMEM((leaves, S), jnp.int32),
            pltpu.VMEM((node_count, S, 2 * S), bf),
            pltpu.VMEM((max(m, 1), S, S), bf),
            pltpu.VMEM((node_count, S, 2 * S), bf),
            pltpu.VMEM((S, leaves * S), bf),
            pltpu.VMEM((leaves * S, CHUNK), bf),
            pltpu.VMEM((pack, 2 * S), bf),
            pltpu.VMEM((peers, pack, S), bf),
            pltpu.VMEM((height, S), bf),
            pltpu.VMEM((2, S, S), bf),
            pltpu.VMEM((R * Q, S, PIECE), bf),
            pltpu.VMEM((R * Q, S, PIECE), bf),
            pltpu.VMEM((R * Q, S, PIECE), bf),
            pltpu.VMEM((Q + EARLY, height, PIECE), bf),
            pltpu.VMEM((Q + EARLY, height, PIECE), bf),
            pltpu.VMEM((max(EARLY, 1), pack, PIECE), bf),
            pltpu.VMEM((max(EARLY, 1), pack, PIECE), bf),
            dma((R * H + 2 + leaves + node_count + m,)),
            dma((R * Q,)),
            dma((R * Q,)),
            dma((R * Q,)),
            dma((R * Q,)),
            dma((peers, max(L, 1))),
            dma((peers, max(L, 1))),
            dma((Q + EARLY, peers)),
            dma((Q + EARLY, peers)),
            dma((max(EARLY, 1),)),
            dma((max(EARLY, 1),)),
            pltpu.SemaphoreType.REGULAR((max(L - 1, 1),)),
        ],
        compiler_params=pltpu.CompilerParams(collective_id=0, has_side_effects=True,
                                             vmem_limit_bytes=60 * 1024 * 1024),
    )(charges, leaf_coef, leaf_rows, local_interp, top_interp)
    return pl.pallas_call(
        store,
        out_shape=(jax.ShapeDtypeStruct((S, width), bf), jax.ShapeDtypeStruct((pack, width), bf)),
        in_specs=[vmem, vmem],
        out_specs=(any_spec, any_spec),
        scratch_shapes=[pltpu.SemaphoreType.DMA((2,))],
        compiler_params=pltpu.CompilerParams(vmem_limit_bytes=4 * 1024 * 1024),
    )(*results)


def solution(mesh):
    placed = (
        P(("leaf", "rhs"), None),
        P(("leaf", "rhs"), None, None),
        P(("leaf", "rhs"), None),
        P("leaf", None, None),
        P("leaf", None),
    )
    return jax.shard_map(
        local,
        mesh=mesh,
        in_specs=placed,
        out_specs=(P("leaf", "rhs"), P("leaf", "rhs")),
        check_vma=False,
    )
```

```python
import functools

import jax
import jax.numpy as jnp
from jax import lax
from jax.experimental import pallas as pl
from jax.experimental.pallas import tpu as pltpu
from jax.sharding import PartitionSpec as P

PIECE = 128
CHUNK = 256
LAG = 2
AHEAD = 3
EARLY = 0
TABLES = 2
WAIT = 3
MESH = pl.DeviceIdType.MESH


def bit(value, k):
    return (value // (1 << k)) % 2


def flip(value, offset, bits):
    out = 0
    for k in range(bits):
        a, b = bit(value, k), bit(offset, k)
        out = out + (a + b - 2 * a * b) * (1 << k)
    return out


def chosen(z, table):
    size = len(table)
    if len(set(table)) == 1:
        return table[0]
    out = 0
    for k, value in enumerate(table):
        differs = ((z - k + size) % size + size - 1) // size
        out = out + (1 - differs) * value
    return out


def dot(a, b):
    return jnp.dot(a, b, preferred_element_type=jnp.float32)


def up_block(R, i):
    return R - 1 - i


def block_order(R, Q, z):
    when = {}
    for c in range(R):
        if c > z:
            when[c] = LAG * z + (R - 1 - c) * Q
        elif c < z:
            when[c] = LAG * (R - 1 - z) + c * Q
        else:
            when[c] = final_step(R, Q, z)
    first = (lambda c: -c) if z < R / 2 else (lambda c: c)
    return sorted(range(R), key=lambda c: (c == z, when[c], first(c)))


def final_step(R, Q, z):
    below = LAG * z + (R - 1 - z) * Q if z > 0 else 0
    above = LAG * (R - 1 - z) + z * Q if z < R - 1 else 0
    return max(below, above)


def segments(S, L, n_leaf):
    out, start = [], 0
    for delta in range(n_leaf):
        first = max(delta.bit_length(), 1)
        rows = (S >> first - 1) - (S >> L)
        padded = -(-rows // 32) * 32
        out.append((start, first, rows, padded))
        start += padded
    return out, start


def kernel(plan, charges, coef, rows, interp, top, root_out, top_out, *scratch):
    (points, mats, picks, nodes, halves, ops, skel, leafw, tops, tables, wide, level_ops, parts,
     below, above, leaving, coming, sums, extra, load_sem, up_send, up_recv, down_send, down_recv,
     table_send, table_recv, part_send, part_recv, sum_send, sum_recv, hello) = scratch
    R, L, H, Q = plan["R"], plan["L"], plan["H"], plan["Q"]
    leaves, S, M = plan["leaves"], plan["S"], plan["M"]
    m, n_leaf, early = plan["m"], plan["n_leaf"], plan["early"]
    pack = top.shape[0]
    total = leaves * R
    bf = jnp.bfloat16
    z = lax.axis_index("rhs")
    p = lax.axis_index("leaf")
    segs, height = segments(S, L, n_leaf)
    orders = [block_order(R, Q, k) for k in range(R)]
    chunks = R * H
    hurried = EARLY if R > 1 else 0
    earliest = min(final_step(R, Q, k) for k in range(R))

    barrier = pltpu.get_barrier_semaphore()
    if R > 1:
        @pl.when(z > 0)
        def _():
            pl.semaphore_signal(barrier, inc=1, device_id={"rhs": z - 1}, device_id_type=MESH)

        @pl.when(z < R - 1)
        def _():
            pl.semaphore_signal(barrier, inc=1, device_id={"rhs": z + 1}, device_id_type=MESH)
    for b in range(L):
        pl.semaphore_signal(barrier, inc=1, device_id={"leaf": flip(p, 1 << b, L)}, device_id_type=MESH)
    neighbours = chosen(z, [(k > 0) + (k < R - 1) for k in range(R)])

    def block(i):
        return chosen(z, [orders[k][i] for k in range(R)])

    def chunk_copy(i):
        column = (block(i // H) * H + i % H) * CHUNK
        return pltpu.make_async_copy(
            charges.at[:, pl.ds(pl.multiple_of(column, CHUNK), CHUNK)], points.at[i], load_sem.at[i])

    copies = [(rows, picks), (coef, mats)]
    lead = len(copies)
    for b in range(m):
        index = total - (total >> early + b) + z // (1 << b + 1)
        copies.append((interp.at[index, :, pl.ds(pl.multiple_of(bit(z, b) * S, S), S)], halves.at[b]))
    where = {}
    for level in range(early, 0, -1):
        count = leaves >> level
        base = len(where)
        for k in range(count):
            where[level, k] = len(where)
        copies.append((interp.at[pl.ds(total - (total >> level - 1) + z * count, count)],
                       nodes.at[pl.ds(base, count)]))
    soon = len(copies)
    copies.append((top, tops))
    loads = [pltpu.make_async_copy(a, b, load_sem.at[chunks + i]) for i, (a, b) in enumerate(copies)]

    for copy in loads[:lead]:
        copy.start()
    chunk_copy(0).start()
    for copy in loads[lead:soon]:
        copy.start()

    def table_copies(delta):
        peer = flip(p, delta, L)
        out = []
        for level in range(segs[delta][1], L + 1):
            part = pl.ds(S - (S >> level - 1), S >> level)
            half = pl.ds(pl.multiple_of(bit(peer, level - 1) * S, S), S)
            out.append(pltpu.make_async_remote_copy(
                src_ref=tops.at[part, half], dst_ref=tables.at[delta - 1, part],
                send_sem=table_send.at[0], recv_sem=table_recv.at[0],
                device_id={"leaf": peer}, device_id_type=MESH))
        return out

    def all_tables():
        every = wide.at[pl.ds(0, sum(segs[delta][2] for delta in range(1, n_leaf)))]
        return pltpu.make_async_remote_copy(
            src_ref=every, dst_ref=every, send_sem=table_send.at[0], recv_sem=table_recv.at[0],
            device_id={"leaf": flip(p, 1, L)}, device_id_type=MESH)

    stages = [[d for d in range(1, n_leaf) if bin(d).count("1") == k] for k in range(L + 1)]

    def table_stage(k):
        if k > 1:
            pl.semaphore_wait(hello.at[k - 2], L)
        else:
            loads[-1].wait()
        if k < L:
            for b in range(L):
                pl.semaphore_signal(hello.at[k - 1], inc=1, device_id={"leaf": flip(p, 1 << b, L)},
                                    device_id_type=MESH)
        for delta in stages[k]:
            for copy in table_copies(delta):
                copy.start()

    def send_up(i):
        return pltpu.make_async_remote_copy(
            src_ref=parts.at[i], dst_ref=below.at[i], send_sem=up_send.at[i // Q], recv_sem=up_recv.at[i - Q],
            device_id={"rhs": z + 1}, device_id_type=MESH)

    def send_down(i):
        return pltpu.make_async_remote_copy(
            src_ref=parts.at[i], dst_ref=above.at[i], send_sem=down_send.at[i // Q], recv_sem=down_recv.at[i],
            device_id={"rhs": z - 1}, device_id_type=MESH)

    def whole_block(c, up):
        ref = pl.ds(c * Q, Q)
        return pltpu.make_async_remote_copy(
            src_ref=parts.at[ref], dst_ref=(below if up else above).at[ref],
            send_sem=(up_send if up else down_send).at[c], recv_sem=(up_recv if up else down_recv).at[0],
            device_id={"rhs": z + 1 if up else z - 1}, device_id_type=MESH)

    def part_copy(q, delta):
        start, _, _, padded = segs[delta]
        ref = pl.ds(start, padded)
        return pltpu.make_async_remote_copy(
            src_ref=leaving.at[q, ref], dst_ref=coming.at[q, ref], send_sem=part_send.at[q],
            recv_sem=part_recv.at[q], device_id={"leaf": flip(p, delta, L)}, device_id_type=MESH)

    if hurried:
        @pl.when(chosen(z, [int(k in (1, R - 2)) for k in range(R)]) == 0)
        def _():
            extra[...] = jnp.zeros_like(extra)

    def all_parts(q):
        ref = pl.ds(segs[1][0], height - segs[1][0])
        return pltpu.make_async_remote_copy(
            src_ref=leaving.at[q, ref], dst_ref=coming.at[q, ref], send_sem=part_send.at[q],
            recv_sem=part_recv.at[q], device_id={"leaf": flip(p, 1, L)}, device_id_type=MESH)

    @pl.when(z == 0)
    def _():
        for q in range(Q):
            below[q] = jnp.zeros((S, PIECE), bf)

    @pl.when(z == R - 1)
    def _():
        for q in range(Q):
            above[(R - 1) * Q + q] = jnp.zeros((S, PIECE), bf)

    for copy in loads[:lead]:
        copy.wait()
    lanes = lax.broadcasted_iota(jnp.int32, (S, 128), 1)
    for n in range(leaves):
        across = jnp.transpose(jnp.broadcast_to(picks[n:n + 1, :], (128, S)))
        for t in range(M // 128):
            part = slice(t * 128, (t + 1) * 128)
            mats[n, :, part] = (mats[n, :, part].astype(jnp.float32)
                                + jnp.where(across == lanes + t * 128, 1.0, 0.0)).astype(bf)
    for copy in loads[lead:soon]:
        copy.wait()
    chunk_copy(0).wait()
    loads[-1].start()
    for i in range(1, chunks):
        chunk_copy(i).start()

    def leaf_stage(i):
        if i > 0:
            chunk_copy(i).wait()
        for n in range(leaves):
            leafw[n * S:(n + 1) * S, :] = dot(mats[n], points[i, n * M:(n + 1) * M, :]).astype(bf)

    def compose():
        op = None
        for b in range(m):
            if b == 0:
                op = halves[0]
            else:
                op = dot(halves[b], op).astype(bf)
        current = [op]
        for level in range(early, 0, -1):
            following = []
            for k in range(leaves >> level):
                matrix = nodes[where[level, k]]
                value = matrix if current[k] is None else dot(current[k], matrix).astype(bf)
                if level == 1:
                    skel[:, 2 * k * S:(2 * k + 2) * S] = value
                else:
                    ops[where[level, k]] = value
                    following += [ops[where[level, k], :, :S], ops[where[level, k], :, S:]]
            current = following
        if early == 0:
            rows_at = lax.broadcasted_iota(jnp.int32, (S, S), 0)
            same = jnp.where(rows_at == lax.broadcasted_iota(jnp.int32, (S, S), 1), 1.0, 0.0).astype(bf)
            skel[...] = same if op is None else op

    def chunk(i):
        leaf_stage(i)
        if i == 0:
            compose()
        value = dot(skel[...], leafw[...]).astype(bf)
        c = block(i // H)
        base = c * Q + i % H * (CHUNK // PIECE)
        for j in range(CHUNK // PIECE):
            parts[base + j] = value[:, j * PIECE:(j + 1) * PIECE]
        if i == 0:
            pl.semaphore_wait(barrier, neighbours + L)
        if i < chunks - H and R > 1:
            @pl.when(z == 0)
            def _():
                for j in range(CHUNK // PIECE):
                    send_up(base + j).start()

            @pl.when(z == R - 1)
            def _():
                for j in range(CHUNK // PIECE):
                    send_down(base + j).start()
        if i == 0:
            table_stage(1)

    def prepare_top():
        if n_leaf > 1:
            all_tables().wait_recv()
        for level in range(1, L + 1):
            offset, count = S - (S >> level - 1), S >> level
            half = pl.ds(pl.multiple_of(bit(p, level - 1) * S, S), S)
            for delta in range(1 << level):
                if delta == 0:
                    rows_of = tops[offset:offset + count, half]
                else:
                    rows_of = tables[delta - 1, offset:offset + count, :]
                if level == 1:
                    put_top(level, delta, rows_of)
                else:
                    level_ops[1, delta * count:(delta + 1) * count, :] = rows_of
            if level > 1:
                value = dot(level_ops[1], level_ops[0]).astype(bf)
                for delta in range(1 << level):
                    put_top(level, delta, value[delta * count:(delta + 1) * count])

    def put_top(level, delta, value):
        start, first, _, _ = segs[delta]
        offset, count = (S >> first - 1) - (S >> level - 1), S >> level
        wide[start + offset:start + offset + count, :] = value
        if level < L:
            place = flip(p, delta, L) % (1 << level)
            level_ops[0, pl.ds(pl.multiple_of(place * count, count), count), :] = value

    def add_into(i, other):
        parts[i] = (parts[i].astype(jnp.float32) + other[i].astype(jnp.float32)).astype(bf)

    def any_device(test):
        return any(test(k) for k in range(R))

    def step(t):
        if any_device(lambda k: k > 0 and 0 <= t - LAG * k < (R - 1 - k) * Q):
            s = t - LAG * z

            @pl.when((z > 0) & (s >= 0) & (s < (R - 1 - z) * Q))
            def _():
                i = (R - 1 - s // Q) * Q + s % Q
                send_up(i).wait_recv()
                add_into(i, below)
                send_up(i).start()

        if any_device(lambda k: k < R - 1 and 0 <= t - LAG * (R - 1 - k) < k * Q):
            s_down = t - LAG * (R - 1 - z)

            @pl.when((z < R - 1) & (s_down >= 0) & (s_down < z * Q))
            def _():
                send_down(s_down).wait_recv()
                add_into(s_down, above)
                send_down(s_down).start()

        finals = [final_step(R, Q, k) for k in range(R)]
        if any_device(lambda k: 0 <= t - finals[k] < Q):
            q = t - chosen(z, finals)
            last = chosen(z, [Q - hurried * late(k) for k in range(R)])

            @pl.when((q >= 0) & (q < last))
            def _():
                finish(q)

        for j in range(hurried):
            q = Q - hurried + j
            if any_device(lambda k: late(k) and t == hurry_step(k, q)):
                now = chosen(z, [late(k) * (t == hurry_step(k, q)) for k in range(R)])

                @pl.when(now == 1)
                def _():
                    hurry(q)

    def finish(q):
        i = z * Q + q
        if R > 1:
            @pl.when(z > 0)
            def _():
                send_up(i).wait_recv()

            @pl.when(z < R - 1)
            def _():
                send_down(i).wait_recv()
        root = (parts[i].astype(jnp.float32) + below[i].astype(jnp.float32)
                + above[i].astype(jnp.float32)).astype(bf)
        root_out[:, pl.ds(pl.multiple_of(q * PIECE, PIECE), PIECE)] = root
        spread(q, root)

    def spread(q, value):
        leaving[q] = dot(wide[...], value).astype(bf)
        for delta in sorted(range(1, n_leaf), key=lambda d: (-bin(d >> 1).count("1"), -d)):
            part_copy(q, delta).start()

    def late(k):
        return int(R > 1 and k in (1, R - 2))

    def hurry_step(k, q):
        other = LAG * (R - 1 - k) + k * Q if k == 1 else LAG * k + (R - 1 - k) * Q
        return max((other if R > 2 else 0) + q, final_step(R, Q, k) + Q - hurried - 1)

    def hurry(q):
        i = z * Q + q

        @pl.when(z == 1)
        def _():
            if R > 2:
                send_down(i).wait_recv()
            add_into(i, above)

        @pl.when(z == R - 2)
        def _():
            if R > 2:
                send_up(i).wait_recv()
            add_into(i, below)

        spread(q, parts[i])

    def sum_copy(j, upward):
        return pltpu.make_async_remote_copy(
            src_ref=sums.at[j], dst_ref=extra.at[j], send_sem=sum_send.at[j], recv_sem=sum_recv.at[j],
            device_id={"rhs": z + 1 if upward else z - 1}, device_id_type=MESH)

    def gather(q):
        if n_leaf > 1:
            all_parts(q).wait_recv()
        out = []
        for level in range(1, L + 1):
            offset, count = S - (S >> level - 1), S >> level
            value = None
            for delta in range(1 << level):
                start, first, _, _ = segs[delta]
                at = start + (S >> first - 1) - (S >> level - 1)
                source = leaving if delta == 0 else coming
                term = source[q, at:at + count, :].astype(jnp.float32)
                value = term if value is None else value + term
            out.append((offset, count, value))
        return out

    def end_begin():
        @pl.when((z == 0) | (z == R - 1))
        def _():
            target = chosen(z, [1 if k == 0 else R - 2 for k in range(R)])
            for j in range(hurried):
                spread(Q + j, parts[target * Q + Q - hurried + j])

    def end_finish():
        @pl.when((z == 0) | (z == R - 1))
        def _():
            for j in range(hurried):
                for offset, count, value in gather(Q + j):
                    sums[j, offset:offset + count, :] = value.astype(bf)

        @pl.when(z == 0)
        def _():
            for j in range(hurried):
                sum_copy(j, True).start()

        @pl.when(z == R - 1)
        def _():
            for j in range(hurried):
                sum_copy(j, False).start()

    steps = max(final_step(R, Q, k) for k in range(R)) + Q
    needed = []
    for t in range(steps):
        need = 0
        for k in range(R):
            s, s_down = t - LAG * k, t - LAG * (R - 1 - k)
            blocks = []
            if k > 0 and 0 <= s < (R - 1 - k) * Q:
                blocks.append((R - 1 - s // Q, s % Q))
            if k < R - 1 and 0 <= s_down < k * Q:
                blocks.append((s_down // Q, s_down % Q))
            if 0 <= t - final_step(R, Q, k) < Q:
                blocks.append((k, t - final_step(R, Q, k)))
            for c, q in blocks:
                need = max(need, orders[k].index(c) * H + q // (CHUNK // PIECE) + 1)
        for j in range(hurried):
            q = Q - hurried + j
            for k in range(R):
                if late(k) and t == hurry_step(k, q):
                    need = max(need, orders[k].index(k) * H + q // (CHUNK // PIECE) + 1)
        if t >= earliest:
            need = max(need, chunks if hurried else 0)
        needed.append(need)

    made, stage = 0, 2
    for t in range(steps):
        while made < chunks and (made < needed[t] or made < min(t + AHEAD, chunks)):
            chunk(made)
            made += 1
            if stage <= L and made >= TABLES * (stage - 1):
                table_stage(stage)
                stage += 1
        if t == earliest:
            while stage <= L:
                table_stage(stage)
                stage += 1
            prepare_top()
            if hurried:
                end_begin()
        if hurried and t == earliest + WAIT:
            end_finish()
        step(t)

    if n_leaf > 1:
        all_tables().wait_send()
    if hurried:
        @pl.when((z == 0) | (z == R - 1))
        def _():
            for j in range(hurried):
                all_parts(Q + j).wait_send()

        @pl.when(z == 0)
        def _():
            for j in range(hurried):
                sum_copy(j, True).wait_send()

        @pl.when(z == R - 1)
        def _():
            for j in range(hurried):
                sum_copy(j, False).wait_send()
    if R > 1:
        for c in range(R):
            @pl.when((z < R - 1) & (z < c))
            def _():
                whole_block(c, True).wait_send()

            @pl.when((z > 0) & (z > c))
            def _():
                whole_block(c, False).wait_send()

    for q in range(Q):
        j = q - (Q - hurried)
        if q == Q - 1 and n_leaf > 1:
            for k in range(Q - 1):
                all_parts(k).wait_send()
        columns = slice(q * PIECE, (q + 1) * PIECE)
        values = gather(q)
        if j >= 0:
            i = z * Q + q

            @pl.when(z == 1)
            def _():
                send_up(i).wait_recv()
                root_out[:, columns] = (parts[i].astype(jnp.float32) + below[i].astype(jnp.float32)).astype(bf)
                sum_copy(j, True).wait_recv()

            @pl.when(z == R - 2)
            def _():
                send_down(i).wait_recv()
                root_out[:, columns] = (parts[i].astype(jnp.float32) + above[i].astype(jnp.float32)).astype(bf)
                sum_copy(j, False).wait_recv()
        for offset, count, value in values:
            if j >= 0:
                value = value + extra[j, offset:offset + count, :].astype(jnp.float32)
            top_out[offset:offset + count, columns] = value.astype(bf)

    if n_leaf > 1:
        all_parts(Q - 1).wait_send()


def store(root, top, root_out, top_out, sems):
    copies = [pltpu.make_async_copy(root, root_out, sems.at[0]),
              pltpu.make_async_copy(top, top_out, sems.at[1])]
    for copy in copies:
        copy.start()
    for copy in copies:
        copy.wait()


def local(charges, leaf_coef, leaf_rows, local_interp, top_interp):
    R, n_leaf = lax.axis_size("rhs"), lax.axis_size("leaf")
    leaves, S, M = leaf_coef.shape
    cols = charges.shape[1]
    m, L = R.bit_length() - 1, n_leaf.bit_length() - 1
    early = leaves.bit_length() - 1
    width = cols // R
    H, Q = width // CHUNK, width // PIECE
    plan = dict(R=R, L=L, H=H, Q=Q, leaves=leaves, S=S, M=M, m=m, n_leaf=n_leaf, early=early)
    bf = jnp.bfloat16
    pack = top_interp.shape[0]
    _, height = segments(S, L, n_leaf)
    any_spec = pl.BlockSpec(memory_space=pl.ANY)
    vmem = pl.BlockSpec(memory_space=pltpu.VMEM)
    node_count = max(leaves - 1, 1)
    peers = max(n_leaf - 1, 1)
    dma = pltpu.SemaphoreType.DMA
    results = pl.pallas_call(
        functools.partial(kernel, plan),
        out_shape=(pltpu.VMEM((S, width), bf), pltpu.VMEM((pack, width), bf)),
        in_specs=[pl.BlockSpec(memory_space=pltpu.HBM)] * 5,
        out_specs=(vmem, vmem),
        scratch_shapes=[
            pltpu.VMEM((R * H, leaves * M, CHUNK), bf),
            pltpu.VMEM((leaves, S, M), bf),
            pltpu.VMEM((leaves, S), jnp.int32),
            pltpu.VMEM((node_count, S, 2 * S), bf),
            pltpu.VMEM((max(m, 1), S, S), bf),
            pltpu.VMEM((node_count, S, 2 * S), bf),
            pltpu.VMEM((S, leaves * S), bf),
            pltpu.VMEM((leaves * S, CHUNK), bf),
            pltpu.VMEM((pack, 2 * S), bf),
            pltpu.VMEM((peers, pack, S), bf),
            pltpu.VMEM((height, S), bf),
            pltpu.VMEM((2, S, S), bf),
            pltpu.VMEM((R * Q, S, PIECE), bf),
            pltpu.VMEM((R * Q, S, PIECE), bf),
            pltpu.VMEM((R * Q, S, PIECE), bf),
            pltpu.VMEM((Q + EARLY, height, PIECE), bf),
            pltpu.VMEM((Q + EARLY, height, PIECE), bf),
            pltpu.VMEM((max(EARLY, 1), pack, PIECE), bf),
            pltpu.VMEM((max(EARLY, 1), pack, PIECE), bf),
            dma((R * H + 3 + early + m,)),
            dma((R,)),
            dma((max(R - 1, 1) * Q,)),
            dma((R,)),
            dma((max(R - 1, 1) * Q,)),
            dma((1,)),
            dma((1,)),
            dma((Q + EARLY,)),
            dma((Q + EARLY,)),
            dma((max(EARLY, 1),)),
            dma((max(EARLY, 1),)),
            pltpu.SemaphoreType.REGULAR((max(L - 1, 1),)),
        ],
        compiler_params=pltpu.CompilerParams(collective_id=0, has_side_effects=True,
                                             vmem_limit_bytes=60 * 1024 * 1024),
    )(charges, leaf_coef, leaf_rows, local_interp, top_interp)
    return pl.pallas_call(
        store,
        out_shape=(jax.ShapeDtypeStruct((S, width), bf), jax.ShapeDtypeStruct((pack, width), bf)),
        in_specs=[vmem, vmem],
        out_specs=(any_spec, any_spec),
        scratch_shapes=[pltpu.SemaphoreType.DMA((2,))],
        compiler_params=pltpu.CompilerParams(vmem_limit_bytes=4 * 1024 * 1024),
    )(*results)


def solution(mesh):
    placed = (
        P(("leaf", "rhs"), None),
        P(("leaf", "rhs"), None, None),
        P(("leaf", "rhs"), None),
        P("leaf", None, None),
        P("leaf", None),
    )
    return jax.shard_map(
        local,
        mesh=mesh,
        in_specs=placed,
        out_specs=(P("leaf", "rhs"), P("leaf", "rhs")),
        check_vma=False,
    )
```

```python
import functools

import jax
import jax.numpy as jnp
from jax import lax
from jax.experimental import pallas as pl
from jax.experimental.pallas import tpu as pltpu
from jax.sharding import PartitionSpec as P

PIECE = 128
CHUNK = 256
LAG = 2
AHEAD = 3
EARLY = 0
TABLES = 2
WAIT = 3
MESH = pl.DeviceIdType.MESH


def bit(value, k):
    return (value // (1 << k)) % 2


def flip(value, offset, bits):
    out = 0
    for k in range(bits):
        a, b = bit(value, k), bit(offset, k)
        out = out + (a + b - 2 * a * b) * (1 << k)
    return out


def chosen(z, table):
    size = len(table)
    if len(set(table)) == 1:
        return table[0]
    out = 0
    for k, value in enumerate(table):
        differs = ((z - k + size) % size + size - 1) // size
        out = out + (1 - differs) * value
    return out


def dot(a, b):
    return jnp.dot(a, b, preferred_element_type=jnp.float32)


def up_block(R, i):
    return R - 1 - i


def block_order(R, Q, z):
    when = {}
    for c in range(R):
        if c > z:
            when[c] = LAG * z + (R - 1 - c) * Q
        elif c < z:
            when[c] = LAG * (R - 1 - z) + c * Q
        else:
            when[c] = final_step(R, Q, z)
    first = (lambda c: -c) if z < R / 2 else (lambda c: c)
    return sorted(range(R), key=lambda c: (c == z, when[c], first(c)))


def final_step(R, Q, z):
    below = LAG * z + (R - 1 - z) * Q if z > 0 else 0
    above = LAG * (R - 1 - z) + z * Q if z < R - 1 else 0
    return max(below, above)


def segments(S, L, n_leaf):
    out, start = [], 0
    for delta in range(n_leaf):
        first = max(delta.bit_length(), 1)
        rows = (S >> first - 1) - (S >> L)
        padded = -(-rows // 32) * 32
        out.append((start, first, rows, padded))
        start += padded
    return out, start


def kernel(plan, charges, coef, rows, interp, top, root_out, top_out, *scratch):
    (points, mats, picks, nodes, halves, ops, skel, leafw, tops, tables, wide, level_ops, parts,
     below, above, leaving, coming, sums, extra, load_sem, up_send, up_recv, down_send, down_recv,
     table_send, table_recv, part_send, part_recv, sum_send, sum_recv, hello) = scratch
    R, L, H, Q = plan["R"], plan["L"], plan["H"], plan["Q"]
    leaves, S, M = plan["leaves"], plan["S"], plan["M"]
    m, n_leaf, early = plan["m"], plan["n_leaf"], plan["early"]
    pack = top.shape[0]
    total = leaves * R
    bf = jnp.bfloat16
    z = lax.axis_index("rhs")
    p = lax.axis_index("leaf")
    segs, height = segments(S, L, n_leaf)
    orders = [block_order(R, Q, k) for k in range(R)]
    chunks = R * H
    hurried = EARLY if R > 1 else 0
    earliest = min(final_step(R, Q, k) for k in range(R))

    barrier = pltpu.get_barrier_semaphore()
    if R > 1:
        @pl.when(z > 0)
        def _():
            pl.semaphore_signal(barrier, inc=1, device_id={"rhs": z - 1}, device_id_type=MESH)

        @pl.when(z < R - 1)
        def _():
            pl.semaphore_signal(barrier, inc=1, device_id={"rhs": z + 1}, device_id_type=MESH)
    for b in range(L):
        pl.semaphore_signal(barrier, inc=1, device_id={"leaf": flip(p, 1 << b, L)}, device_id_type=MESH)
    neighbours = chosen(z, [(k > 0) + (k < R - 1) for k in range(R)])

    def block(i):
        return chosen(z, [orders[k][i] for k in range(R)])

    def chunk_copy(i):
        column = (block(i // H) * H + i % H) * CHUNK
        return pltpu.make_async_copy(
            charges.at[:, pl.ds(pl.multiple_of(column, CHUNK), CHUNK)], points.at[i], load_sem.at[i])

    copies = [(rows, picks), (coef, mats)]
    lead = len(copies)
    for b in range(m):
        index = total - (total >> early + b) + z // (1 << b + 1)
        copies.append((interp.at[index, :, pl.ds(pl.multiple_of(bit(z, b) * S, S), S)], halves.at[b]))
    where = {}
    for level in range(early, 0, -1):
        count = leaves >> level
        base = len(where)
        for k in range(count):
            where[level, k] = len(where)
        copies.append((interp.at[pl.ds(total - (total >> level - 1) + z * count, count)],
                       nodes.at[pl.ds(base, count)]))
    soon = len(copies)
    copies.append((top, tops))
    loads = [pltpu.make_async_copy(a, b, load_sem.at[chunks + i]) for i, (a, b) in enumerate(copies)]

    for copy in loads[:lead]:
        copy.start()
    for copy in loads[lead:soon]:
        copy.start()
    chunk_copy(0).start()

    def table_copies(delta):
        peer = flip(p, delta, L)
        out = []
        for level in range(segs[delta][1], L + 1):
            part = pl.ds(S - (S >> level - 1), S >> level)
            half = pl.ds(pl.multiple_of(bit(peer, level - 1) * S, S), S)
            out.append(pltpu.make_async_remote_copy(
                src_ref=tops.at[part, half], dst_ref=tables.at[delta - 1, part],
                send_sem=table_send.at[0], recv_sem=table_recv.at[0],
                device_id={"leaf": peer}, device_id_type=MESH))
        return out

    def all_tables():
        every = wide.at[pl.ds(0, sum(segs[delta][2] for delta in range(1, n_leaf)))]
        return pltpu.make_async_remote_copy(
            src_ref=every, dst_ref=every, send_sem=table_send.at[0], recv_sem=table_recv.at[0],
            device_id={"leaf": flip(p, 1, L)}, device_id_type=MESH)

    stages = [[d for d in range(1, n_leaf) if bin(d).count("1") == k] for k in range(L + 1)]

    def table_stage(k):
        if k > 1:
            pl.semaphore_wait(hello.at[k - 2], L)
        else:
            loads[-1].wait()
        if k < L:
            for b in range(L):
                pl.semaphore_signal(hello.at[k - 1], inc=1, device_id={"leaf": flip(p, 1 << b, L)},
                                    device_id_type=MESH)
        for delta in stages[k]:
            for copy in table_copies(delta):
                copy.start()

    def send_up(i):
        return pltpu.make_async_remote_copy(
            src_ref=parts.at[i], dst_ref=below.at[i], send_sem=up_send.at[i // Q], recv_sem=up_recv.at[i - Q],
            device_id={"rhs": z + 1}, device_id_type=MESH)

    def send_down(i):
        return pltpu.make_async_remote_copy(
            src_ref=parts.at[i], dst_ref=above.at[i], send_sem=down_send.at[i // Q], recv_sem=down_recv.at[i],
            device_id={"rhs": z - 1}, device_id_type=MESH)

    def whole_block(c, up):
        ref = pl.ds(c * Q, Q)
        return pltpu.make_async_remote_copy(
            src_ref=parts.at[ref], dst_ref=(below if up else above).at[ref],
            send_sem=(up_send if up else down_send).at[c], recv_sem=(up_recv if up else down_recv).at[0],
            device_id={"rhs": z + 1 if up else z - 1}, device_id_type=MESH)

    def part_copy(q, delta):
        start, _, _, padded = segs[delta]
        ref = pl.ds(start, padded)
        return pltpu.make_async_remote_copy(
            src_ref=leaving.at[q, ref], dst_ref=coming.at[q, ref], send_sem=part_send.at[q],
            recv_sem=part_recv.at[q], device_id={"leaf": flip(p, delta, L)}, device_id_type=MESH)

    if hurried:
        @pl.when(chosen(z, [int(k in (1, R - 2)) for k in range(R)]) == 0)
        def _():
            extra[...] = jnp.zeros_like(extra)

    def all_parts(q):
        ref = pl.ds(segs[1][0], height - segs[1][0])
        return pltpu.make_async_remote_copy(
            src_ref=leaving.at[q, ref], dst_ref=coming.at[q, ref], send_sem=part_send.at[q],
            recv_sem=part_recv.at[q], device_id={"leaf": flip(p, 1, L)}, device_id_type=MESH)

    @pl.when(z == 0)
    def _():
        for q in range(Q):
            below[q] = jnp.zeros((S, PIECE), bf)

    @pl.when(z == R - 1)
    def _():
        for q in range(Q):
            above[(R - 1) * Q + q] = jnp.zeros((S, PIECE), bf)

    def leaf_stage(i):
        if i > 0:
            chunk_copy(i).wait()
        for n in range(leaves):
            leafw[n * S:(n + 1) * S, :] = dot(mats[n], points[i, n * M:(n + 1) * M, :]).astype(bf)

    def compose():
        op = None
        for b in range(m):
            if b == 0:
                op = halves[0]
            else:
                op = dot(halves[b], op).astype(bf)
        current = [op]
        for level in range(early, 0, -1):
            following = []
            for k in range(leaves >> level):
                matrix = nodes[where[level, k]]
                value = matrix if current[k] is None else dot(current[k], matrix).astype(bf)
                if level == 1:
                    skel[:, 2 * k * S:(2 * k + 2) * S] = value
                else:
                    ops[where[level, k]] = value
                    following += [ops[where[level, k], :, :S], ops[where[level, k], :, S:]]
            current = following
        if early == 0:
            rows_at = lax.broadcasted_iota(jnp.int32, (S, S), 0)
            same = jnp.where(rows_at == lax.broadcasted_iota(jnp.int32, (S, S), 1), 1.0, 0.0).astype(bf)
            skel[...] = same if op is None else op

    def chunk(i):
        leaf_stage(i)
        value = dot(skel[...], leafw[...]).astype(bf)
        c = block(i // H)
        base = c * Q + i % H * (CHUNK // PIECE)
        for j in range(CHUNK // PIECE):
            parts[base + j] = value[:, j * PIECE:(j + 1) * PIECE]
        if i == 0:
            pl.semaphore_wait(barrier, neighbours + L)
        if i < chunks - H and R > 1:
            @pl.when(z == 0)
            def _():
                for j in range(CHUNK // PIECE):
                    send_up(base + j).start()

            @pl.when(z == R - 1)
            def _():
                for j in range(CHUNK // PIECE):
                    send_down(base + j).start()
        if i == 0:
            table_stage(1)

    def prepare_top():
        if n_leaf > 1:
            all_tables().wait_recv()
        for level in range(1, L + 1):
            offset, count = S - (S >> level - 1), S >> level
            half = pl.ds(pl.multiple_of(bit(p, level - 1) * S, S), S)
            for delta in range(1 << level):
                if delta == 0:
                    rows_of = tops[offset:offset + count, half]
                else:
                    rows_of = tables[delta - 1, offset:offset + count, :]
                if level == 1:
                    put_top(level, delta, rows_of)
                else:
                    level_ops[1, delta * count:(delta + 1) * count, :] = rows_of
            if level > 1:
                value = dot(level_ops[1], level_ops[0]).astype(bf)
                for delta in range(1 << level):
                    put_top(level, delta, value[delta * count:(delta + 1) * count])

    def put_top(level, delta, value):
        start, first, _, _ = segs[delta]
        offset, count = (S >> first - 1) - (S >> level - 1), S >> level
        wide[start + offset:start + offset + count, :] = value
        if level < L:
            place = flip(p, delta, L) % (1 << level)
            level_ops[0, pl.ds(pl.multiple_of(place * count, count), count), :] = value

    def add_into(i, other):
        parts[i] = (parts[i].astype(jnp.float32) + other[i].astype(jnp.float32)).astype(bf)

    def any_device(test):
        return any(test(k) for k in range(R))

    def step(t):
        if any_device(lambda k: k > 0 and 0 <= t - LAG * k < (R - 1 - k) * Q):
            s = t - LAG * z

            @pl.when((z > 0) & (s >= 0) & (s < (R - 1 - z) * Q))
            def _():
                i = (R - 1 - s // Q) * Q + s % Q
                send_up(i).wait_recv()
                add_into(i, below)
                send_up(i).start()

        if any_device(lambda k: k < R - 1 and 0 <= t - LAG * (R - 1 - k) < k * Q):
            s_down = t - LAG * (R - 1 - z)

            @pl.when((z < R - 1) & (s_down >= 0) & (s_down < z * Q))
            def _():
                send_down(s_down).wait_recv()
                add_into(s_down, above)
                send_down(s_down).start()

        finals = [final_step(R, Q, k) for k in range(R)]
        if any_device(lambda k: 0 <= t - finals[k] < Q):
            q = t - chosen(z, finals)
            last = chosen(z, [Q - hurried * late(k) for k in range(R)])

            @pl.when((q >= 0) & (q < last))
            def _():
                finish(q)

        for j in range(hurried):
            q = Q - hurried + j
            if any_device(lambda k: late(k) and t == hurry_step(k, q)):
                now = chosen(z, [late(k) * (t == hurry_step(k, q)) for k in range(R)])

                @pl.when(now == 1)
                def _():
                    hurry(q)

    def finish(q):
        i = z * Q + q
        if R > 1:
            @pl.when(z > 0)
            def _():
                send_up(i).wait_recv()

            @pl.when(z < R - 1)
            def _():
                send_down(i).wait_recv()
        root = (parts[i].astype(jnp.float32) + below[i].astype(jnp.float32)
                + above[i].astype(jnp.float32)).astype(bf)
        root_out[:, pl.ds(pl.multiple_of(q * PIECE, PIECE), PIECE)] = root
        spread(q, root)

    def spread(q, value):
        cut = segs[2][0] if n_leaf > 2 else 0
        leaving[q, cut:, :] = dot(wide[cut:, :], value).astype(bf)
        for delta in sorted(range(1, n_leaf), key=lambda d: (-bin(d >> 1).count("1"), -d)):
            if delta == 1 and cut:
                leaving[q, :cut, :] = dot(wide[:cut, :], value).astype(bf)
            part_copy(q, delta).start()

    def late(k):
        return int(R > 1 and k in (1, R - 2))

    def hurry_step(k, q):
        other = LAG * (R - 1 - k) + k * Q if k == 1 else LAG * k + (R - 1 - k) * Q
        return max((other if R > 2 else 0) + q, final_step(R, Q, k) + Q - hurried - 1)

    def hurry(q):
        i = z * Q + q

        @pl.when(z == 1)
        def _():
            if R > 2:
                send_down(i).wait_recv()
            add_into(i, above)

        @pl.when(z == R - 2)
        def _():
            if R > 2:
                send_up(i).wait_recv()
            add_into(i, below)

        spread(q, parts[i])

    def sum_copy(j, upward):
        return pltpu.make_async_remote_copy(
            src_ref=sums.at[j], dst_ref=extra.at[j], send_sem=sum_send.at[j], recv_sem=sum_recv.at[j],
            device_id={"rhs": z + 1 if upward else z - 1}, device_id_type=MESH)

    def gather(q):
        if n_leaf > 1:
            all_parts(q).wait_recv()
        out = []
        for level in range(1, L + 1):
            offset, count = S - (S >> level - 1), S >> level
            value = None
            for delta in range(1 << level):
                start, first, _, _ = segs[delta]
                at = start + (S >> first - 1) - (S >> level - 1)
                source = leaving if delta == 0 else coming
                term = source[q, at:at + count, :].astype(jnp.float32)
                value = term if value is None else value + term
            out.append((offset, count, value))
        return out

    def end_begin():
        @pl.when((z == 0) | (z == R - 1))
        def _():
            target = chosen(z, [1 if k == 0 else R - 2 for k in range(R)])
            for j in range(hurried):
                spread(Q + j, parts[target * Q + Q - hurried + j])

    def end_finish():
        @pl.when((z == 0) | (z == R - 1))
        def _():
            for j in range(hurried):
                for offset, count, value in gather(Q + j):
                    sums[j, offset:offset + count, :] = value.astype(bf)

        @pl.when(z == 0)
        def _():
            for j in range(hurried):
                sum_copy(j, True).start()

        @pl.when(z == R - 1)
        def _():
            for j in range(hurried):
                sum_copy(j, False).start()

    steps = max(final_step(R, Q, k) for k in range(R)) + Q
    needed = []
    for t in range(steps):
        need = 0
        for k in range(R):
            s, s_down = t - LAG * k, t - LAG * (R - 1 - k)
            blocks = []
            if k > 0 and 0 <= s < (R - 1 - k) * Q:
                blocks.append((R - 1 - s // Q, s % Q))
            if k < R - 1 and 0 <= s_down < k * Q:
                blocks.append((s_down // Q, s_down % Q))
            if 0 <= t - final_step(R, Q, k) < Q:
                blocks.append((k, t - final_step(R, Q, k)))
            for c, q in blocks:
                need = max(need, orders[k].index(c) * H + q // (CHUNK // PIECE) + 1)
        for j in range(hurried):
            q = Q - hurried + j
            for k in range(R):
                if late(k) and t == hurry_step(k, q):
                    need = max(need, orders[k].index(k) * H + q // (CHUNK // PIECE) + 1)
        if t >= earliest:
            need = max(need, chunks if hurried else 0)
        needed.append(need)

    for copy in loads[:soon]:
        copy.wait()
    lanes = lax.broadcasted_iota(jnp.int32, (S, 128), 1)
    for n in range(leaves):
        across = jnp.transpose(jnp.broadcast_to(picks[n:n + 1, :], (128, S)))
        for t in range(M // 128):
            part = slice(t * 128, (t + 1) * 128)
            mats[n, :, part] = (mats[n, :, part].astype(jnp.float32)
                                + jnp.where(across == lanes + t * 128, 1.0, 0.0)).astype(bf)
    compose()
    chunk_copy(0).wait()
    loads[-1].start()
    for i in range(1, chunks):
        chunk_copy(i).start()

    made, stage = 0, 2
    for t in range(steps):
        while made < chunks and (made < needed[t] or made < min(t + AHEAD, chunks)):
            chunk(made)
            made += 1
            if stage <= L and made >= TABLES * (stage - 1):
                table_stage(stage)
                stage += 1
        if t == earliest:
            while stage <= L:
                table_stage(stage)
                stage += 1
            prepare_top()
            if hurried:
                end_begin()
        if hurried and t == earliest + WAIT:
            end_finish()
        step(t)

    if n_leaf > 1:
        all_tables().wait_send()
    if hurried:
        @pl.when((z == 0) | (z == R - 1))
        def _():
            for j in range(hurried):
                all_parts(Q + j).wait_send()

        @pl.when(z == 0)
        def _():
            for j in range(hurried):
                sum_copy(j, True).wait_send()

        @pl.when(z == R - 1)
        def _():
            for j in range(hurried):
                sum_copy(j, False).wait_send()
    if R > 1:
        for c in range(R):
            @pl.when((z < R - 1) & (z < c))
            def _():
                whole_block(c, True).wait_send()

            @pl.when((z > 0) & (z > c))
            def _():
                whole_block(c, False).wait_send()

    for q in range(Q):
        j = q - (Q - hurried)
        if q == Q - 1 and n_leaf > 1:
            for k in range(Q - 1):
                all_parts(k).wait_send()
        columns = slice(q * PIECE, (q + 1) * PIECE)
        values = gather(q)
        if j >= 0:
            i = z * Q + q

            @pl.when(z == 1)
            def _():
                send_up(i).wait_recv()
                root_out[:, columns] = (parts[i].astype(jnp.float32) + below[i].astype(jnp.float32)).astype(bf)
                sum_copy(j, True).wait_recv()

            @pl.when(z == R - 2)
            def _():
                send_down(i).wait_recv()
                root_out[:, columns] = (parts[i].astype(jnp.float32) + above[i].astype(jnp.float32)).astype(bf)
                sum_copy(j, False).wait_recv()
        for offset, count, value in values:
            if j >= 0:
                value = value + extra[j, offset:offset + count, :].astype(jnp.float32)
            top_out[offset:offset + count, columns] = value.astype(bf)

    if n_leaf > 1:
        all_parts(Q - 1).wait_send()


def store(root, top, root_out, top_out, sems):
    copies = [pltpu.make_async_copy(root, root_out, sems.at[0]),
              pltpu.make_async_copy(top, top_out, sems.at[1])]
    for copy in copies:
        copy.start()
    for copy in copies:
        copy.wait()


def local(charges, leaf_coef, leaf_rows, local_interp, top_interp):
    R, n_leaf = lax.axis_size("rhs"), lax.axis_size("leaf")
    leaves, S, M = leaf_coef.shape
    cols = charges.shape[1]
    m, L = R.bit_length() - 1, n_leaf.bit_length() - 1
    early = leaves.bit_length() - 1
    width = cols // R
    H, Q = width // CHUNK, width // PIECE
    plan = dict(R=R, L=L, H=H, Q=Q, leaves=leaves, S=S, M=M, m=m, n_leaf=n_leaf, early=early)
    bf = jnp.bfloat16
    pack = top_interp.shape[0]
    _, height = segments(S, L, n_leaf)
    any_spec = pl.BlockSpec(memory_space=pl.ANY)
    vmem = pl.BlockSpec(memory_space=pltpu.VMEM)
    node_count = max(leaves - 1, 1)
    peers = max(n_leaf - 1, 1)
    dma = pltpu.SemaphoreType.DMA
    results = pl.pallas_call(
        functools.partial(kernel, plan),
        out_shape=(pltpu.VMEM((S, width), bf), pltpu.VMEM((pack, width), bf)),
        in_specs=[pl.BlockSpec(memory_space=pltpu.HBM)] * 5,
        out_specs=(vmem, vmem),
        scratch_shapes=[
            pltpu.VMEM((R * H, leaves * M, CHUNK), bf),
            pltpu.VMEM((leaves, S, M), bf),
            pltpu.VMEM((leaves, S), jnp.int32),
            pltpu.VMEM((node_count, S, 2 * S), bf),
            pltpu.VMEM((max(m, 1), S, S), bf),
            pltpu.VMEM((node_count, S, 2 * S), bf),
            pltpu.VMEM((S, leaves * S), bf),
            pltpu.VMEM((leaves * S, CHUNK), bf),
            pltpu.VMEM((pack, 2 * S), bf),
            pltpu.VMEM((peers, pack, S), bf),
            pltpu.VMEM((height, S), bf),
            pltpu.VMEM((2, S, S), bf),
            pltpu.VMEM((R * Q, S, PIECE), bf),
            pltpu.VMEM((R * Q, S, PIECE), bf),
            pltpu.VMEM((R * Q, S, PIECE), bf),
            pltpu.VMEM((Q + EARLY, height, PIECE), bf),
            pltpu.VMEM((Q + EARLY, height, PIECE), bf),
            pltpu.VMEM((max(EARLY, 1), pack, PIECE), bf),
            pltpu.VMEM((max(EARLY, 1), pack, PIECE), bf),
            dma((R * H + 3 + early + m,)),
            dma((R,)),
            dma((max(R - 1, 1) * Q,)),
            dma((R,)),
            dma((max(R - 1, 1) * Q,)),
            dma((1,)),
            dma((1,)),
            dma((Q + EARLY,)),
            dma((Q + EARLY,)),
            dma((max(EARLY, 1),)),
            dma((max(EARLY, 1),)),
            pltpu.SemaphoreType.REGULAR((max(L - 1, 1),)),
        ],
        compiler_params=pltpu.CompilerParams(collective_id=0, has_side_effects=True,
                                             vmem_limit_bytes=60 * 1024 * 1024),
    )(charges, leaf_coef, leaf_rows, local_interp, top_interp)
    return pl.pallas_call(
        store,
        out_shape=(jax.ShapeDtypeStruct((S, width), bf), jax.ShapeDtypeStruct((pack, width), bf)),
        in_specs=[vmem, vmem],
        out_specs=(any_spec, any_spec),
        scratch_shapes=[pltpu.SemaphoreType.DMA((2,))],
        compiler_params=pltpu.CompilerParams(vmem_limit_bytes=4 * 1024 * 1024),
    )(*results)


def solution(mesh):
    placed = (
        P(("leaf", "rhs"), None),
        P(("leaf", "rhs"), None, None),
        P(("leaf", "rhs"), None),
        P("leaf", None, None),
        P("leaf", None),
    )
    return jax.shard_map(
        local,
        mesh=mesh,
        in_specs=placed,
        out_specs=(P("leaf", "rhs"), P("leaf", "rhs")),
        check_vma=False,
    )
```
